32 devices in a mesh: fsdp: 16 (over z, y, x), dp: 2 (over core).
Axes of the slice: x: 2, y: 2, z: 4, core: 2. Of those that a mesh axis runs over, the one named last changes fastest.
Arguments:
- normed: bfloat16 [2, 4096, 4096], P(None, ('fsdp', 'dp')), may hold values from -6 to 6
- kv_cotangent: bfloat16 [2, 4096, 512], P(None, ('fsdp', 'dp')), may hold values from -6 to 6
- kv_weight: bfloat16 [4096, 512], P('fsdp'), may hold values from -0.09375 to 0.09375
- main_grad: float32 [4096, 512], P('fsdp'), may hold values from -6 to 6
- owner_order: int32 [16], replicated, may hold values from 0 to 15, each once
Outputs:
- key_rows: bfloat16 [2, 4096, 512], P(None, ('fsdp', 'dp'))
- input_grad: bfloat16 [2, 4096, 4096], P(None, ('fsdp', 'dp'))
- grad_buffer: float32 [4096, 512], P('fsdp')
The draws below stay inside these ranges and needn't reach their ends.
Inputs may be any that keep to these rules, and one draw needn't show every extreme that they name: `owner_order`: a permutation: each value appears once.
All inputs are finite; a program needn't handle non-finite values.
Results may differ from the reference program's by a relative error of at most 0.0075.
Values may be sent and summed in bfloat16 or wider, within the bound.
A program may use at most 64 MiB of HBM per device.

```python
import math
import jax
import jax.numpy as jnp
from jax import lax

D = 4096
MICRO = 2
TOK_DEV = 128
KVW = 512
TOKENS = 4096
N_FSDP = 16
N_DP = 2


def steps_of(rng, dims, split, smallest, high):
    level = 1.0
    for axis_at, blocks in split:
        heights = jax.random.uniform(jax.random.fold_in(jax.random.fold_in(rng, 6), axis_at), (blocks,), jnp.float32, smallest / len(split), high / len(split))
        level = level * jnp.repeat(jnp.exp(heights), dims[axis_at] // blocks).reshape((-1,) + (1,) * (len(dims) - 1 - axis_at))
    return level


def gaussian(rng, shape, scale, reach, cuts=(), kind=jnp.bfloat16):
    level = steps_of(rng, shape, cuts, -0.22, 0.18) if cuts else 1.0
    array = jax.random.normal(rng, shape, jnp.float32) * scale * level
    return jnp.minimum(jnp.maximum(array, -reach), reach).astype(kind)


def setup_inputs(seed: int = 0) -> dict:
    key_list = jax.random.split(jax.random.key(seed), 6)
    normed = gaussian(key_list[0], (MICRO, TOKENS, D), 1.0, 6.0, ((1, 32),))
    kv_cotangent = gaussian(key_list[1], (MICRO, TOKENS, KVW), 1.0, 6.0, ((1, 32),))
    kv_weight = gaussian(key_list[2], (D, KVW), D ** -0.5, 0.09375, ((0, 16),))
    main_grad = gaussian(key_list[3], (D, KVW), 1.0, 6.0, ((0, 16),), jnp.float32)
    owner_order = jax.random.permutation(key_list[4], N_FSDP).astype(jnp.int32)
    return dict(normed=normed, kv_cotangent=kv_cotangent, kv_weight=kv_weight, main_grad=main_grad, owner_order=owner_order)


def reference(normed, kv_cotangent, kv_weight, main_grad, owner_order):
    shard_rows = D // N_FSDP
    block_count = MICRO * N_DP
    block_rows = TOK_DEV * N_FSDP
    inverse_owner = jnp.argsort(owner_order).astype(jnp.int32)
    blocks_in = normed.reshape(block_count, block_rows, D)
    blocks_cot = kv_cotangent.reshape(block_count, block_rows, KVW)

    def advance(grad_sum, inputs_pair):
        inputs, cotangent = inputs_pair
        permuted = inputs.reshape(block_rows, N_FSDP, shard_rows)[:, owner_order, :].reshape(block_rows, D)
        key_block = jnp.dot(permuted, kv_weight, preferred_element_type=jnp.float32).astype(jnp.bfloat16)
        grad_permuted = jnp.dot(cotangent, kv_weight.T, preferred_element_type=jnp.float32).astype(jnp.bfloat16)
        grad_block = grad_permuted.reshape(block_rows, N_FSDP, shard_rows)[:, inverse_owner, :].reshape(block_rows, D)
        grad_sum = grad_sum + jnp.dot(permuted.T, cotangent, preferred_element_type=jnp.float32)
        return (grad_sum, (key_block, grad_block))
    grad_sum, outputs = lax.scan(advance, jnp.zeros((D, KVW), jnp.float32), (blocks_in, blocks_cot))
    key_blocks, grad_blocks = outputs
    grad_scale = 1.0 / math.sqrt(MICRO * TOKENS)
    grad_buffer = main_grad + grad_sum * grad_scale
    return (key_blocks.reshape(MICRO, TOKENS, KVW), grad_blocks.reshape(MICRO, TOKENS, D), grad_buffer)
```

```python
import functools
import math

import jax
import jax.numpy as jnp
from jax import lax
from jax.experimental import pallas as pl
from jax.experimental.pallas import tpu as pltpu
from jax.sharding import PartitionSpec as P

MESH = pl.DeviceIdType.MESH
F32 = jnp.float32
BF16 = jnp.bfloat16


def kernel(
    n, dp, chunk, scale,
    x_hbm, c_hbm, w_hbm, main_hbm,
    key_hbm, ig_hbm, gb_hbm,
    xx, cc, ck, gath, part, r1, t1, r2, t2, r3, fin, main, gb, key, ig, acc,
    load_sem, out_sem, send_sem, x_recv, az_recv, a1_recv, a2_recv, ad_recv, r1_recv, r2_recv, r3_recv, rd_recv,
):
    f = lax.axis_index("fsdp")
    d = lax.axis_index("dp")
    k = lax.rem(d, 2)
    sib = d + 1 - 2 * k
    rows, width = x_hbm.shape
    key_width = c_hbm.shape[1]
    half = key_width // 2
    depth = n // 4
    chunks = width // chunk
    z = lax.div(f, 4)
    low = lax.rem(f, 4)
    bit0 = lax.rem(low, 2)
    bit1 = lax.div(low, 2)
    flip_x = low + 1 - 2 * bit0
    flip_y = low + 2 - 4 * bit1
    low1 = flip_x + k * (flip_y - flip_x)
    low2 = flip_y + k * (flip_x - flip_y)
    low12 = 3 - low
    p1 = z * 4 + low1
    p2 = z * 4 + low2
    steps = sorted(range(1, depth), key=lambda s: (min(s, depth - s), s))

    def peer(s):
        return lax.rem(z + s, depth)

    def dev(fi, di):
        return {"fsdp": fi, "dp": di}

    loads = []

    def load(src, dst, i):
        cp = pltpu.make_async_copy(src, dst, load_sem.at[i])
        cp.start()
        loads.append(cp)

    load(w_hbm.at[:, pl.ds(0, half)], gath.at[0, f], 0)
    load(w_hbm.at[:, pl.ds(half, half)], gath.at[1, f], 1)
    load(c_hbm, cc.at[0], 2)
    load(x_hbm, xx.at[0], 3)
    load(main_hbm, main, 4)

    barrier = pltpu.get_barrier_semaphore()
    greeted = [dev(peer(s) * 4 + low, d) for s in steps]
    greeted += [dev(p1, d), dev(p2, d)]
    greeted += [dev(f, lax.rem(d + s, dp)) for s in range(1, dp)]
    for g in greeted:
        pl.semaphore_signal(barrier, inc=1, device_id=g, device_id_type=MESH)
    pl.semaphore_wait(barrier, len(greeted))

    sent = []

    def send(src, dst, rsem, to):
        cp = pltpu.make_async_remote_copy(
            src_ref=src, dst_ref=dst, send_sem=send_sem, recv_sem=rsem, device_id=to, device_id_type=MESH
        )
        cp.start()
        sent.append(cp)

    def arrived(dst, rsem, frm):
        pltpu.make_async_remote_copy(
            src_ref=dst, dst_ref=dst, send_sem=send_sem, recv_sem=rsem, device_id=frm, device_id_type=MESH
        ).wait_recv()

    to_sib = dev(f, sib)
    to1 = dev(p1, d)
    to2 = dev(p2, d)

    send(x_hbm, xx.at[1], x_recv.at[0], to_sib)
    send(c_hbm, cc.at[1], x_recv.at[1], to_sib)
    loads[0].wait()
    loads[1].wait()

    def block(fi):
        return gath.at[k, fi]

    send(block(f), block(f), a1_recv.at[z], to1)
    send(block(f), block(f), a2_recv.at[z], to2)
    for s in steps:
        send(block(f), block(f), az_recv.at[z], dev(peer(s) * 4 + low, d))

    loads[2].wait()
    loads[3].wait()
    arrived(cc.at[1], x_recv.at[1], to_sib)
    arrived(xx.at[1], x_recv.at[0], to_sib)
    side = pl.ds(pl.multiple_of(k * half, half), half)
    ck[...] = cc[:, :, side].reshape(2 * rows, half)

    per = chunk // part.shape[1]
    ring = steps + [0]
    blockwise = per == 1

    def partial(cols):
        both = xx[:, :, cols].reshape(2 * rows, chunk)
        prod = lax.dot_general(both, ck[...], (((0,), (0,)), ((), ())), preferred_element_type=F32)
        return prod.astype(BF16)

    def feature_block(fb):
        return pl.ds(pl.multiple_of(fb * chunk, chunk), chunk)

    def partials(lo):
        if blockwise:
            for s in ring:
                fb = peer(s) * 4 + lo
                part[fb] = partial(feature_block(fb))
                if lo is low12:
                    send(part.at[fb], r1.at[0, peer(s)], r1_recv.at[0, peer(s)], to1)
                if lo is low1:
                    send(part.at[fb], r1.at[1, peer(s)], r1_recv.at[1, peer(s)], to1)

    if not blockwise:
        for j in range(chunks):
            made = partial(pl.ds(j * chunk, chunk))
            part[j * per : (j + 1) * per] = made.reshape(per, part.shape[1], half)
        for s in ring:
            send(part.at[peer(s) * 4 + low12], r1.at[0, peer(s)], r1_recv.at[0, peer(s)], to1)
    partials(low12)
    for s in steps:
        zb = peer(s)
        fb = zb * 4 + low
        arrived(block(fb), az_recv.at[zb], dev(fb, d))
        send(block(fb), block(fb), a1_recv.at[zb], to1)
        send(block(fb), block(fb), a2_recv.at[zb], to2)
        send(block(fb), block(fb), ad_recv.at[fb], to_sib)
    if not blockwise:
        for s in ring:
            send(part.at[peer(s) * 4 + low1], r1.at[1, peer(s)], r1_recv.at[1, peer(s)], to1)
    partials(low1)
    partials(low2)
    partials(low)

    outs = []

    def put(src, dst, i):
        cp = pltpu.make_async_copy(src, dst, out_sem.at[i])
        cp.start()
        outs.append(cp)

    contract = (((1,), (1,)), ((), ()))

    def from_sib(lo):
        for s in [0] + steps:
            fb = peer(s) * 4 + lo
            if s or lo is not low:
                arrived(gath.at[1 - k, fb], ad_recv.at[fb], to_sib)

    def use(lo):
        if not blockwise:
            return
        from_sib(lo)
        for s in [0] + steps:
            fb = peer(s) * 4 + lo
            cols = feature_block(fb)
            w0 = gath[0, fb]
            w1 = gath[1, fb]
            prod = lax.dot_general(cc[0, :, :half], w0, contract, preferred_element_type=F32)
            prod = prod + lax.dot_general(cc[0, :, half:], w1, contract, preferred_element_type=F32)
            ig[:, cols] = prod.astype(BF16)
            put(ig.at[:, cols], ig_hbm.at[:, cols], len(outs))
            xb = xx[0, :, cols]
            k0 = jnp.dot(xb, w0, preferred_element_type=F32)
            k1 = jnp.dot(xb, w1, preferred_element_type=F32)
            if s == 0 and lo is low:
                acc[:, :half] = k0
                acc[:, half:] = k1
            else:
                acc[:, :half] += k0
                acc[:, half:] += k1

    for s in [0] + steps:
        zb = peer(s)
        fb = zb * 4 + low1
        arrived(block(fb), a1_recv.at[zb], to1)
        send(block(fb), block(fb), a2_recv.at[depth + zb], to2)
        send(block(fb), block(fb), ad_recv.at[fb], to_sib)
    for s in ring:
        zb = peer(s)
        arrived(r1.at[0, zb], r1_recv.at[0, zb], to1)
        t1[zb] = (part[zb * 4 + low2].astype(F32) + r1[0, zb].astype(F32)).astype(BF16)
        send(t1.at[zb], r2.at[zb], r2_recv.at[zb], to2)
    use(low)
    for s in steps:
        zb = peer(s)
        arrived(r1.at[1, zb], r1_recv.at[1, zb], to1)
        arrived(r2.at[zb], r2_recv.at[zb], to2)
        t2[zb] = (part[zb * 4 + low].astype(F32) + r1[1, zb].astype(F32) + r2[zb].astype(F32)).astype(BF16)
        send(t2.at[zb], r3.at[z], r3_recv.at[z], dev(zb * 4 + low, d))
    for s in [0] + steps:
        zb = peer(s)
        fb = zb * 4 + low2
        arrived(block(fb), a2_recv.at[zb], to2)
        send(block(fb), block(fb), ad_recv.at[fb], to_sib)
    use(low1)
    use(low2)
    for s in [0] + steps:
        zb = peer(s)
        fb = zb * 4 + low12
        arrived(block(fb), a2_recv.at[depth + zb], to2)
        send(block(fb), block(fb), ad_recv.at[fb], to_sib)

    arrived(r1.at[1, z], r1_recv.at[1, z], to1)
    arrived(r2.at[z], r2_recv.at[z], to2)
    total = part[f].astype(F32) + r1[1, z].astype(F32) + r2[z].astype(F32)
    for s in steps:
        arrived(r3.at[peer(s)], r3_recv.at[peer(s)], dev(peer(s) * 4 + low, d))
        total = total + r3[peer(s)].astype(F32)
    fin[d] = total
    for s in range(1, dp):
        send(fin.at[d], fin.at[d], rd_recv.at[d], dev(f, lax.rem(d + s, dp)))

    use(low12)
    if blockwise:
        key[...] = acc[...].astype(BF16)
    else:
        for lo in (low, low1, low2, low12):
            from_sib(lo)
        for j in range(chunks):
            w0 = gath[0, j * per : (j + 1) * per].reshape(chunk, half)
            w1 = gath[1, j * per : (j + 1) * per].reshape(chunk, half)
            prod = lax.dot_general(cc[0, :, :half], w0, contract, preferred_element_type=F32)
            prod = prod + lax.dot_general(cc[0, :, half:], w1, contract, preferred_element_type=F32)
            ig[:, j * chunk : (j + 1) * chunk] = prod.astype(BF16)
        put(ig, ig_hbm, 0)
        for h in range(2):
            w = gath[h].reshape(width, half)
            key[:, h * half : (h + 1) * half] = jnp.dot(xx[0], w, preferred_element_type=F32).astype(BF16)
    put(key, key_hbm, len(outs))

    for s in range(1, dp):
        src = lax.rem(d + s, dp)
        arrived(fin.at[src], rd_recv.at[src], dev(f, src))
    loads[4].wait()
    for h in range(2):
        total = fin[h]
        for g in range(1, dp // 2):
            total = total + fin[2 * g + h]
        cols = slice(h * half, (h + 1) * half)
        gb[:, cols] = main[:, cols] + total * scale
    put(gb, gb_hbm, len(outs))
    for cp in sent:
        cp.wait_send()
    for cp in outs:
        cp.wait()


def reorder_kernel(depth, scatter, order_ref, x_ref, y_ref):
    for j in range(x_ref.shape[1] // depth):
        here = slice(j * depth, (j + 1) * depth)
        there = pl.ds(pl.multiple_of(order_ref[j] * depth, depth), depth)
        if scatter:
            y_ref[:, there] = x_ref[:, here]
        else:
            y_ref[:, here] = x_ref[:, there]


def reorder(x, order, scatter):
    rows, width = x.shape
    n = order.shape[0]
    depth = width // n
    if depth % 128:
        if scatter:
            order = jnp.argsort(order)
        return jnp.take(x.reshape(rows, n, depth), order, axis=1, mode="clip").reshape(rows, width)
    tile = rows // 4
    spec = pl.BlockSpec((tile, width), lambda i: (i, 0))
    return pl.pallas_call(
        functools.partial(reorder_kernel, depth, scatter),
        grid=(rows // tile,),
        out_shape=jax.ShapeDtypeStruct((rows, width), x.dtype),
        in_specs=[pl.BlockSpec(memory_space=pltpu.SMEM), spec],
        out_specs=spec,
        cost_estimate=pl.CostEstimate(flops=0, bytes_accessed=4 * rows * width, transcendentals=0),
    )(order, x)


def exchange(
    n, dp, scale,
    order_hbm, x_hbm, c_hbm, w_hbm, main_hbm,
    key, ig, gb, order,
    xx, cc, ck, gath, mine, give, take, part, r1, hop, zin, t3, r3, fin, main, acc,
    load_sem, send_sem, ag_recv, sib_recv, take_recv, r1_recv, z_recv, r3_recv, fin_recv,
):
    f = lax.axis_index("fsdp")
    d = lax.axis_index("dp")
    k = lax.rem(d, 2)
    sib = d + 1 - 2 * k
    chunk, key_width = main_hbm.shape
    half = key_width // 2
    depth = n // 4
    z = lax.div(f, 4)
    low = lax.rem(f, 4)
    bit0 = lax.rem(low, 2)
    bit1 = lax.div(low, 2)
    flip0 = low + 1 - 2 * bit0
    flip1 = low + 2 - 4 * bit1
    low_a = flip0 + k * (flip1 - flip0)
    low_b = flip1 + k * (flip0 - flip1)
    low_ab = 3 - low
    upper = lax.div(2 * z, depth)
    has_up = z < depth - 1
    has_dn = z > 0
    mid = jnp.logical_and(has_up, has_dn)

    def far(t):
        return (1 - upper) * (depth - 1 - t) + upper * t

    def close(i):
        up = i + jnp.where(i >= z, 1, 0)
        dn = depth - 1 - i - jnp.where(depth - 1 - i <= z, 1, 0)
        return (1 - upper) * up + upper * dn

    def dev(fi, di):
        return {"fsdp": fi, "dp": di}

    to_a = dev(z * 4 + low_a, d)
    to_b = dev(z * 4 + low_b, d)
    to_sib = dev(f, sib)

    def level(zi):
        return dev(lax.rem(zi + depth, depth) * 4 + low, d)

    loads = []

    def load(src, dst):
        cp = pltpu.make_async_copy(src, dst, load_sem.at[len(loads)])
        cp.start()
        loads.append(cp)

    load(w_hbm.at[:, pl.ds(0, half)], gath.at[0, f])
    load(w_hbm.at[:, pl.ds(half, half)], gath.at[1, f])
    load(order_hbm, order)
    load(c_hbm, cc)
    for j in range(n):
        load(x_hbm.at[:, pl.ds(j * chunk, chunk)], xx.at[j])
    load(main_hbm, main)
    load_x = loads[4 : 4 + n]

    barrier = pltpu.get_barrier_semaphore()

    def greet(to):
        pl.semaphore_signal(barrier, inc=1, device_id=to, device_id_type=MESH)

    greet(to_a)
    greet(to_b)
    for s in range(1, dp):
        greet(dev(f, lax.rem(d + s, dp)))

    @pl.when(has_up)
    def _():
        greet(level(z + 1))

    @pl.when(has_dn)
    def _():
        greet(level(z - 1))

    pl.semaphore_wait(barrier, dp + 1 + jnp.where(has_up, 1, 0) + jnp.where(has_dn, 1, 0))

    sent = []

    def send(src, dst, rsem, to, cond=None):
        cp = pltpu.make_async_remote_copy(
            src_ref=src, dst_ref=dst, send_sem=send_sem, recv_sem=rsem, device_id=to, device_id_type=MESH
        )
        if cond is None:
            cp.start()
        else:
            pl.when(cond)(cp.start)
        return cp, cond

    def post(*args):
        sent.append(send(*args))

    def arrived(dst, rsem):
        pltpu.make_async_remote_copy(
            src_ref=dst, dst_ref=dst, send_sem=send_sem, recv_sem=rsem, device_id=to_sib, device_id_type=MESH
        ).wait_recv()

    def block(fb):
        return gath.at[k, fb]

    def forward(fb, to, cond=None):
        send(block(fb), block(fb), ag_recv.at[fb], to, cond)

    def forward_sib(fb):
        send(block(fb), block(fb), sib_recv.at[fb], to_sib)

    contract_rows = (((0,), (0,)), ((), ()))
    contract_cols = (((1,), (1,)), ((), ()))

    def partial(lo, t):
        fb = far(t) * 4 + lo
        prod = lax.dot_general(xx[order[fb]], ck[...], contract_rows, preferred_element_type=F32)
        give[fb] = prod[:, half:].astype(BF16)
        send(give.at[fb], take.at[fb], take_recv.at[fb], to_sib)
        mine[fb] = prod[:, :half]

    def pair(fb):
        return mine[fb] + take[fb].astype(F32)

    def across(j, t):
        zz = far(t)
        fb = zz * 4 + (low_ab if j else low_b)
        arrived(take.at[fb], take_recv.at[fb])
        part[fb] = pair(fb).astype(BF16)
        send(part.at[fb], r1.at[j, zz], r1_recv.at[j, zz], to_b)

    def from_a():
        fb = z * 4 + low_a
        arrived(block(fb), ag_recv.at[fb])
        forward(fb, level(z + 1), has_up)
        forward(fb, level(z - 1), has_dn)
        forward_sib(fb)

    def from_z(i, j):
        zz = close(i)
        fb = zz * 4 + (low_a if j else low)
        arrived(block(fb), ag_recv.at[fb])
        below = zz < z
        on = jnp.logical_or(jnp.logical_and(below, has_up), jnp.logical_and(zz > z, has_dn))
        forward(fb, level(z + jnp.where(below, 1, -1)), on)
        forward(fb, to_b)
        forward_sib(fb)

    def from_b(zz, j):
        fb = zz * 4 + (low_ab if j else low_b)
        arrived(block(fb), ag_recv.at[fb])
        forward_sib(fb)

    def ready(j, zz):
        fb = zz * 4 + (low_a if j else low)
        arrived(take.at[fb], take_recv.at[fb])
        arrived(r1.at[j, zz], r1_recv.at[j, zz])
        return pair(fb) + r1[j, zz].astype(F32)

    def along(t, j):
        zz = far(t)

        @pl.when(zz != z)
        def _():
            side = jnp.where(zz > z, 0, 1)
            edge = jnp.where(zz > z, z == 0, z == depth - 1)

            @pl.when(jnp.logical_not(edge))
            def _():
                arrived(zin.at[side, zz, j], z_recv.at[side, zz, j])

            total = ready(j, zz) + zin[side, zz, j].astype(F32)
            hop[j, zz] = total.astype(BF16)
            send(hop.at[j, zz], zin.at[side, zz, j], z_recv.at[side, zz, j], level(z + 1 - 2 * side))

    def settle(j):
        total = ready(j, z)

        @pl.when(has_dn)
        def _():
            arrived(zin.at[0, z, j], z_recv.at[0, z, j])

        @pl.when(has_up)
        def _():
            arrived(zin.at[1, z, j], z_recv.at[1, z, j])

        return total + zin[0, z, j].astype(F32) + zin[1, z, j].astype(F32)

    def use(fb, first=False):
        w0 = gath[0, fb]
        w1 = gath[1, fb]
        prod = lax.dot_general(cc[:, :half], w0, contract_cols, preferred_element_type=F32)
        prod = prod + lax.dot_general(cc[:, half:], w1, contract_cols, preferred_element_type=F32)
        ig[fb] = prod.astype(BF16)
        xb = xx[order[fb]]
        k0 = jnp.dot(xb, w0, preferred_element_type=F32)
        k1 = jnp.dot(xb, w1, preferred_element_type=F32)
        if first:
            acc[:, :half] = k0
            acc[:, half:] = k1
        else:
            acc[:, :half] += k0
            acc[:, half:] += k1

    def use_when(zz, lo):
        fb = zz * 4 + lo
        arrived(gath.at[1 - k, fb], sib_recv.at[fb])
        use(fb)

    loads[0].wait()
    loads[1].wait()
    forward(f, to_a)
    forward(f, level(z + 1), has_up)
    forward(f, level(z - 1), has_dn)

    @pl.when(z == 0)
    def _():
        zin[0] = jnp.zeros(zin.shape[1:], BF16)

    @pl.when(z == depth - 1)
    def _():
        zin[1] = jnp.zeros(zin.shape[1:], BF16)

    loads[3].wait()
    ck[:, :half] = cc[:, pl.ds(pl.multiple_of(k * half, half), half)]
    ck[:, half:] = cc[:, pl.ds(pl.multiple_of((1 - k) * half, half), half)]
    loads[2].wait()
    for cp in load_x:
        cp.wait()

    steps = []
    for t in range(depth):
        steps += [
            functools.partial(partial, low_ab, t),
            functools.partial(partial, low_a, t),
            functools.partial(partial, low_b, t),
        ]
    sends = []
    for t in range(depth):
        sends += [functools.partial(across, 1, t), functools.partial(across, 0, t)]
    LAG = 3
    due = {}
    for s, fn in enumerate(sends):
        due.setdefault(LAG + (3 * s) // 2, []).append(fn)
    due.setdefault(5, []).append(from_a)
    due.setdefault(6, []).append(lambda: forward(f, to_b))

    def first_z():
        from_z(0, 0)

        @pl.when(mid)
        def _():
            from_z(1, 0)

    due.setdefault(9, []).append(first_z)
    due.setdefault(10, []).append(lambda: forward(z * 4 + low_a, to_b))
    last = max(max(due), len(steps) - 1)
    for m in range(last + 1):
        if m < len(steps):
            steps[m]()
        for fn in due.get(m, []):
            fn()

    def rest(ends):
        along(0, 1) if ends else None
        partial(low, 0)
        along(0, 0) if ends else None
        partial(low, 1)
        from_z(0, 1)
        if not ends:
            from_z(1, 1)
        partial(low, 2)
        along(1, 1) if ends else None
        partial(low, 3)
        use(f, True)
        from_b(z, 0)
        if ends:
            from_z(1, 0)
            use_when(close(0), low)
            along(1, 0)
            from_b(z, 1)
            use_when(z, low_b)
            from_z(1, 1)
            along(2, 1)
            use_when(close(1), low)
            from_b(close(0), 0)
            from_z(2, 0)
            along(2, 0)
            use_when(z, low_a)
            from_b(close(0), 1)
            use_when(z, low_ab)
            from_z(2, 1)
            from_b(close(1), 0)
        else:
            from_z(2, 0)
            along(0, 1)
            use_when(close(0), low)
            use_when(close(1), low)
            from_b(z, 1)
            from_z(2, 1)
            along(0, 0)
            use_when(z, low_b)
            along(3, 1)
            from_b(close(0), 0)
            use_when(z, low_a)
            along(1, 1)
            use_when(z, low_ab)
            from_b(close(1), 0)
            along(3, 0)
            along(1, 0)
            from_b(close(0), 1)

    @pl.when(mid)
    def _():
        rest(False)

    @pl.when(jnp.logical_not(mid))
    def _():
        rest(True)

    use_when(close(2), low)
    use_when(close(0), low_b)
    use_when(close(0), low_a)
    t3[...] = settle(1).astype(BF16)
    send(t3, r3, r3_recv, to_a)
    from_b(close(1), 1)
    use_when(close(1), low_b)
    use_when(close(1), low_a)
    use_when(close(0), low_ab)
    total = settle(0)
    arrived(r3, r3_recv)
    fin[d] = total + r3[...].astype(F32)
    for s in range(1, dp):
        send(fin.at[d], fin.at[d], fin_recv.at[d], dev(f, lax.rem(d + s, dp)))
    from_b(close(2), 0)
    use_when(close(1), low_ab)
    use_when(close(2), low_b)
    from_b(close(2), 1)
    use_when(close(2), low_a)
    loads[-1].wait()
    for s in range(1, dp):
        src = lax.rem(d + s, dp)
        arrived(fin.at[src], fin_recv.at[src])
    for h in range(2):
        total = fin[h]
        for g in range(1, dp // 2):
            total = total + fin[2 * g + h]
        side = slice(h * half, (h + 1) * half)
        gb[:, side] = main[:, side] + total * scale
    use_when(close(2), low_ab)
    key[...] = acc[...].astype(BF16)

    per_z = jnp.where(has_up, z + 1, 0) + jnp.where(has_dn, depth - z, 0)
    blocks = 4 + 6 * (depth - 1) + 8 * depth + 1 + 2 * per_z

    def left(_, carry):
        send_done(give.at[f])
        return carry

    def send_done(src):
        pltpu.make_async_remote_copy(
            src_ref=src, dst_ref=src, send_sem=send_sem, recv_sem=r3_recv, device_id=to_sib, device_id_type=MESH
        ).wait_send()

    lax.fori_loop(0, blocks, left, 0)
    for s in range(1, dp):
        send_done(fin.at[d])


def place(order, key, ig, gb, key_hbm, ig_hbm, gb_hbm, sem):
    n, _, chunk = ig.shape
    puts = []
    for fb in range(n):
        there = pl.ds(pl.multiple_of(order[fb] * chunk, chunk), chunk)
        puts.append(pltpu.make_async_copy(ig.at[fb], ig_hbm.at[:, there], sem.at[fb]))
    puts.append(pltpu.make_async_copy(key, key_hbm, sem.at[n]))
    puts.append(pltpu.make_async_copy(gb, gb_hbm, sem.at[n + 1]))
    for cp in puts:
        cp.start()
    for cp in puts:
        cp.wait()


def near(x, c, w, main, order, n, dp, scale):
    rows, width = x.shape
    chunk, key_width = main.shape
    half = key_width // 2
    depth = n // 4
    dma = pltpu.SemaphoreType.DMA
    block = (chunk, half)
    hbm = pl.BlockSpec(memory_space=pltpu.HBM)
    smem = pl.BlockSpec(memory_space=pltpu.SMEM)
    vmem = pl.BlockSpec(memory_space=pltpu.VMEM)
    operands = [pltpu.with_memory_space_constraint(a, pltpu.HBM) for a in (order, x, c, w, main)]
    key, ig, gb, order = pl.pallas_call(
        functools.partial(exchange, n, dp, scale),
        out_shape=(
            pltpu.VMEM((rows, key_width), BF16),
            pltpu.VMEM((n, rows, chunk), BF16),
            pltpu.VMEM((chunk, key_width), F32),
            pltpu.SMEM((n,), jnp.int32),
        ),
        in_specs=[hbm] * 5,
        out_specs=(vmem,) * 3 + (smem,),
        scratch_shapes=[
            pltpu.VMEM((n, rows, chunk), BF16),
            pltpu.VMEM((rows, key_width), BF16),
            pltpu.VMEM((rows, key_width), BF16),
            pltpu.VMEM((2, n) + block, BF16),
            pltpu.VMEM((n,) + block, F32),
            pltpu.VMEM((n,) + block, BF16),
            pltpu.VMEM((n,) + block, BF16),
            pltpu.VMEM((n,) + block, BF16),
            pltpu.VMEM((2, depth) + block, BF16),
            pltpu.VMEM((2, depth) + block, BF16),
            pltpu.VMEM((2, depth, 2) + block, BF16),
            pltpu.VMEM(block, BF16),
            pltpu.VMEM(block, BF16),
            pltpu.VMEM((dp,) + block, F32),
            pltpu.VMEM((chunk, key_width), F32),
            pltpu.VMEM((rows, key_width), F32),
            dma((n + 5,)),
            dma,
            dma((n,)),
            dma((n,)),
            dma((n,)),
            dma((2, depth)),
            dma((2, depth, 2)),
            dma,
            dma((dp,)),
        ],
        compiler_params=pltpu.CompilerParams(
            collective_id=0, has_side_effects=True, vmem_limit_bytes=36 * 1024 * 1024
        ),
    )(*operands)
    return pl.pallas_call(
        place,
        out_shape=(
            jax.ShapeDtypeStruct((rows, key_width), BF16),
            jax.ShapeDtypeStruct((rows, width), BF16),
            jax.ShapeDtypeStruct((chunk, key_width), F32),
        ),
        in_specs=[smem] + [vmem] * 3,
        out_specs=(hbm,) * 3,
        scratch_shapes=[dma((n + 2,))],
        compiler_params=pltpu.CompilerParams(vmem_limit_bytes=8 * 1024 * 1024),
    )(order, key, ig, gb)


def body(normed, kv_cotangent, kv_weight, main_grad, owner_order):
    micro_count, tok_dev, width = normed.shape
    shard_rows, key_width = kv_weight.shape
    n = lax.axis_size("fsdp")
    dp = lax.axis_size("dp")
    rows = micro_count * tok_dev
    half = key_width // 2
    depth = n // 4
    scale = 1.0 / math.sqrt(rows * n * dp)
    chunk = shard_rows if shard_rows % 128 == 0 else max(shard_rows, 256)
    if depth == 4 and shard_rows % 128 == 0:
        key, ig, gb = near(
            normed.reshape(rows, width), kv_cotangent.reshape(rows, key_width), kv_weight, main_grad, owner_order, n, dp, scale
        )
        return (
            key.reshape(micro_count, tok_dev, key_width),
            ig.reshape(micro_count, tok_dev, width),
            gb,
        )
    x = reorder(normed.reshape(rows, width), owner_order, False)
    chunks = width // chunk
    dma = pltpu.SemaphoreType.DMA
    half_block = (shard_rows, half)
    any_spec = pl.BlockSpec(memory_space=pl.ANY)
    key, ig, gb = pl.pallas_call(
        functools.partial(kernel, n, dp, chunk, scale),
        out_shape=(
            jax.ShapeDtypeStruct((rows, key_width), BF16),
            jax.ShapeDtypeStruct((rows, width), BF16),
            jax.ShapeDtypeStruct((shard_rows, key_width), F32),
        ),
        in_specs=[any_spec] * 4,
        out_specs=(any_spec,) * 3,
        scratch_shapes=[
            pltpu.VMEM((2, rows, width), BF16),
            pltpu.VMEM((2, rows, key_width), BF16),
            pltpu.VMEM((2 * rows, half), BF16),
            pltpu.VMEM((2, n) + half_block, BF16),
            pltpu.VMEM((n,) + half_block, BF16),
            pltpu.VMEM((2, depth) + half_block, BF16),
            pltpu.VMEM((depth,) + half_block, BF16),
            pltpu.VMEM((depth,) + half_block, BF16),
            pltpu.VMEM((depth,) + half_block, BF16),
            pltpu.VMEM((depth,) + half_block, BF16),
            pltpu.VMEM((dp,) + half_block, F32),
            pltpu.VMEM((shard_rows, key_width), F32),
            pltpu.VMEM((shard_rows, key_width), F32),
            pltpu.VMEM((rows, key_width), BF16),
            pltpu.VMEM((rows, width), BF16),
            pltpu.VMEM((rows, key_width), F32),
            dma((5,)),
            dma((chunks + 2,)),
            dma,
            dma((2,)),
            dma((depth,)),
            dma((depth,)),
            dma((2 * depth,)),
            dma((n,)),
            dma((2, depth)),
            dma((depth,)),
            dma((depth,)),
            dma((dp,)),
        ],
        compiler_params=pltpu.CompilerParams(
            collective_id=0, has_side_effects=True
        ),
    )(x, kv_cotangent.reshape(rows, key_width), kv_weight, main_grad)
    ig = reorder(ig, owner_order, True)
    return (
        key.reshape(micro_count, tok_dev, key_width),
        ig.reshape(micro_count, tok_dev, width),
        gb,
    )


def solution(mesh):
    in_specs = (
        P(None, ("fsdp", "dp"), None),
        P(None, ("fsdp", "dp"), None),
        P("fsdp", None),
        P("fsdp", None),
        P(),
    )
    out_specs = (P(None, ("fsdp", "dp"), None), P(None, ("fsdp", "dp"), None), P("fsdp", None))
    return jax.shard_map(body, mesh=mesh, in_specs=in_specs, out_specs=out_specs, check_vma=False)
```

```python
import functools
import math

import jax
import jax.numpy as jnp
from jax import lax
from jax.experimental import pallas as pl
from jax.experimental.pallas import tpu as pltpu
from jax.sharding import PartitionSpec as P

MESH = pl.DeviceIdType.MESH
F32 = jnp.float32
BF16 = jnp.bfloat16


def kernel(
    n, dp, chunk, scale,
    x_hbm, c_hbm, w_hbm, main_hbm,
    key_hbm, ig_hbm, gb_hbm,
    xx, cc, ck, gath, part, r1, t1, r2, t2, r3, fin, main, gb, key, ig, acc,
    load_sem, out_sem, send_sem, x_recv, az_recv, a1_recv, a2_recv, ad_recv, r1_recv, r2_recv, r3_recv, rd_recv,
):
    f = lax.axis_index("fsdp")
    d = lax.axis_index("dp")
    k = lax.rem(d, 2)
    sib = d + 1 - 2 * k
    rows, width = x_hbm.shape
    key_width = c_hbm.shape[1]
    half = key_width // 2
    depth = n // 4
    chunks = width // chunk
    z = lax.div(f, 4)
    low = lax.rem(f, 4)
    bit0 = lax.rem(low, 2)
    bit1 = lax.div(low, 2)
    flip_x = low + 1 - 2 * bit0
    flip_y = low + 2 - 4 * bit1
    low1 = flip_x + k * (flip_y - flip_x)
    low2 = flip_y + k * (flip_x - flip_y)
    low12 = 3 - low
    p1 = z * 4 + low1
    p2 = z * 4 + low2
    steps = sorted(range(1, depth), key=lambda s: (min(s, depth - s), s))

    def peer(s):
        return lax.rem(z + s, depth)

    def dev(fi, di):
        return {"fsdp": fi, "dp": di}

    loads = []

    def load(src, dst, i):
        cp = pltpu.make_async_copy(src, dst, load_sem.at[i])
        cp.start()
        loads.append(cp)

    load(w_hbm.at[:, pl.ds(0, half)], gath.at[0, f], 0)
    load(w_hbm.at[:, pl.ds(half, half)], gath.at[1, f], 1)
    load(c_hbm, cc.at[0], 2)
    load(x_hbm, xx.at[0], 3)
    load(main_hbm, main, 4)

    barrier = pltpu.get_barrier_semaphore()
    greeted = [dev(peer(s) * 4 + low, d) for s in steps]
    greeted += [dev(p1, d), dev(p2, d)]
    greeted += [dev(f, lax.rem(d + s, dp)) for s in range(1, dp)]
    for g in greeted:
        pl.semaphore_signal(barrier, inc=1, device_id=g, device_id_type=MESH)
    pl.semaphore_wait(barrier, len(greeted))

    sent = []

    def send(src, dst, rsem, to):
        cp = pltpu.make_async_remote_copy(
            src_ref=src, dst_ref=dst, send_sem=send_sem, recv_sem=rsem, device_id=to, device_id_type=MESH
        )
        cp.start()
        sent.append(cp)

    def arrived(dst, rsem, frm):
        pltpu.make_async_remote_copy(
            src_ref=dst, dst_ref=dst, send_sem=send_sem, recv_sem=rsem, device_id=frm, device_id_type=MESH
        ).wait_recv()

    to_sib = dev(f, sib)
    to1 = dev(p1, d)
    to2 = dev(p2, d)

    send(x_hbm, xx.at[1], x_recv.at[0], to_sib)
    send(c_hbm, cc.at[1], x_recv.at[1], to_sib)
    loads[0].wait()
    loads[1].wait()

    def block(fi):
        return gath.at[k, fi]

    send(block(f), block(f), a1_recv.at[z], to1)
    send(block(f), block(f), a2_recv.at[z], to2)
    for s in steps:
        send(block(f), block(f), az_recv.at[z], dev(peer(s) * 4 + low, d))

    loads[2].wait()
    loads[3].wait()
    arrived(cc.at[1], x_recv.at[1], to_sib)
    arrived(xx.at[1], x_recv.at[0], to_sib)
    side = pl.ds(pl.multiple_of(k * half, half), half)
    ck[...] = cc[:, :, side].reshape(2 * rows, half)

    per = chunk // part.shape[1]
    ring = steps + [0]
    blockwise = per == 1

    def partial(cols):
        both = xx[:, :, cols].reshape(2 * rows, chunk)
        prod = lax.dot_general(both, ck[...], (((0,), (0,)), ((), ())), preferred_element_type=F32)
        return prod.astype(BF16)

    def feature_block(fb):
        return pl.ds(pl.multiple_of(fb * chunk, chunk), chunk)

    def partials(lo):
        if blockwise:
            for s in ring:
                fb = peer(s) * 4 + lo
                part[fb] = partial(feature_block(fb))
                if lo is low12:
                    send(part.at[fb], r1.at[0, peer(s)], r1_recv.at[0, peer(s)], to1)
                if lo is low1:
                    send(part.at[fb], r1.at[1, peer(s)], r1_recv.at[1, peer(s)], to1)

    if not blockwise:
        for j in range(chunks):
            made = partial(pl.ds(j * chunk, chunk))
            part[j * per : (j + 1) * per] = made.reshape(per, part.shape[1], half)
        for s in ring:
            send(part.at[peer(s) * 4 + low12], r1.at[0, peer(s)], r1_recv.at[0, peer(s)], to1)
    partials(low12)
    for s in steps:
        zb = peer(s)
        fb = zb * 4 + low
        arrived(block(fb), az_recv.at[zb], dev(fb, d))
        send(block(fb), block(fb), a1_recv.at[zb], to1)
        send(block(fb), block(fb), a2_recv.at[zb], to2)
        send(block(fb), block(fb), ad_recv.at[fb], to_sib)
    if not blockwise:
        for s in ring:
            send(part.at[peer(s) * 4 + low1], r1.at[1, peer(s)], r1_recv.at[1, peer(s)], to1)
    partials(low1)
    partials(low2)
    partials(low)

    outs = []

    def put(src, dst, i):
        cp = pltpu.make_async_copy(src, dst, out_sem.at[i])
        cp.start()
        outs.append(cp)

    contract = (((1,), (1,)), ((), ()))

    def from_sib(lo):
        for s in [0] + steps:
            fb = peer(s) * 4 + lo
            if s or lo is not low:
                arrived(gath.at[1 - k, fb], ad_recv.at[fb], to_sib)

    def use(lo):
        if not blockwise:
            return
        from_sib(lo)
        for s in [0] + steps:
            fb = peer(s) * 4 + lo
            cols = feature_block(fb)
            w0 = gath[0, fb]
            w1 = gath[1, fb]
            prod = lax.dot_general(cc[0, :, :half], w0, contract, preferred_element_type=F32)
            prod = prod + lax.dot_general(cc[0, :, half:], w1, contract, preferred_element_type=F32)
            ig[:, cols] = prod.astype(BF16)
            put(ig.at[:, cols], ig_hbm.at[:, cols], len(outs))
            xb = xx[0, :, cols]
            k0 = jnp.dot(xb, w0, preferred_element_type=F32)
            k1 = jnp.dot(xb, w1, preferred_element_type=F32)
            if s == 0 and lo is low:
                acc[:, :half] = k0
                acc[:, half:] = k1
            else:
                acc[:, :half] += k0
                acc[:, half:] += k1

    for s in [0] + steps:
        zb = peer(s)
        fb = zb * 4 + low1
        arrived(block(fb), a1_recv.at[zb], to1)
        send(block(fb), block(fb), a2_recv.at[depth + zb], to2)
        send(block(fb), block(fb), ad_recv.at[fb], to_sib)
    for s in ring:
        zb = peer(s)
        arrived(r1.at[0, zb], r1_recv.at[0, zb], to1)
        t1[zb] = (part[zb * 4 + low2].astype(F32) + r1[0, zb].astype(F32)).astype(BF16)
        send(t1.at[zb], r2.at[zb], r2_recv.at[zb], to2)
    use(low)
    for s in steps:
        zb = peer(s)
        arrived(r1.at[1, zb], r1_recv.at[1, zb], to1)
        arrived(r2.at[zb], r2_recv.at[zb], to2)
        t2[zb] = (part[zb * 4 + low].astype(F32) + r1[1, zb].astype(F32) + r2[zb].astype(F32)).astype(BF16)
        send(t2.at[zb], r3.at[z], r3_recv.at[z], dev(zb * 4 + low, d))
    for s in [0] + steps:
        zb = peer(s)
        fb = zb * 4 + low2
        arrived(block(fb), a2_recv.at[zb], to2)
        send(block(fb), block(fb), ad_recv.at[fb], to_sib)
    use(low1)
    use(low2)
    for s in [0] + steps:
        zb = peer(s)
        fb = zb * 4 + low12
        arrived(block(fb), a2_recv.at[depth + zb], to2)
        send(block(fb), block(fb), ad_recv.at[fb], to_sib)

    arrived(r1.at[1, z], r1_recv.at[1, z], to1)
    arrived(r2.at[z], r2_recv.at[z], to2)
    total = part[f].astype(F32) + r1[1, z].astype(F32) + r2[z].astype(F32)
    for s in steps:
        arrived(r3.at[peer(s)], r3_recv.at[peer(s)], dev(peer(s) * 4 + low, d))
        total = total + r3[peer(s)].astype(F32)
    fin[d] = total
    for s in range(1, dp):
        send(fin.at[d], fin.at[d], rd_recv.at[d], dev(f, lax.rem(d + s, dp)))

    use(low12)
    if blockwise:
        key[...] = acc[...].astype(BF16)
    else:
        for lo in (low, low1, low2, low12):
            from_sib(lo)
        for j in range(chunks):
            w0 = gath[0, j * per : (j + 1) * per].reshape(chunk, half)
            w1 = gath[1, j * per : (j + 1) * per].reshape(chunk, half)
            prod = lax.dot_general(cc[0, :, :half], w0, contract, preferred_element_type=F32)
            prod = prod + lax.dot_general(cc[0, :, half:], w1, contract, preferred_element_type=F32)
            ig[:, j * chunk : (j + 1) * chunk] = prod.astype(BF16)
        put(ig, ig_hbm, 0)
        for h in range(2):
            w = gath[h].reshape(width, half)
            key[:, h * half : (h + 1) * half] = jnp.dot(xx[0], w, preferred_element_type=F32).astype(BF16)
    put(key, key_hbm, len(outs))

    for s in range(1, dp):
        src = lax.rem(d + s, dp)
        arrived(fin.at[src], rd_recv.at[src], dev(f, src))
    loads[4].wait()
    for h in range(2):
        total = fin[h]
        for g in range(1, dp // 2):
            total = total + fin[2 * g + h]
        cols = slice(h * half, (h + 1) * half)
        gb[:, cols] = main[:, cols] + total * scale
    put(gb, gb_hbm, len(outs))
    for cp in sent:
        cp.wait_send()
    for cp in outs:
        cp.wait()


def reorder_kernel(depth, scatter, order_ref, x_ref, y_ref):
    for j in range(x_ref.shape[1] // depth):
        here = slice(j * depth, (j + 1) * depth)
        there = pl.ds(pl.multiple_of(order_ref[j] * depth, depth), depth)
        if scatter:
            y_ref[:, there] = x_ref[:, here]
        else:
            y_ref[:, here] = x_ref[:, there]


def reorder(x, order, scatter):
    rows, width = x.shape
    n = order.shape[0]
    depth = width // n
    if depth % 128:
        if scatter:
            order = jnp.argsort(order)
        return jnp.take(x.reshape(rows, n, depth), order, axis=1, mode="clip").reshape(rows, width)
    tile = rows // 4
    spec = pl.BlockSpec((tile, width), lambda i: (i, 0))
    return pl.pallas_call(
        functools.partial(reorder_kernel, depth, scatter),
        grid=(rows // tile,),
        out_shape=jax.ShapeDtypeStruct((rows, width), x.dtype),
        in_specs=[pl.BlockSpec(memory_space=pltpu.SMEM), spec],
        out_specs=spec,
        cost_estimate=pl.CostEstimate(flops=0, bytes_accessed=4 * rows * width, transcendentals=0),
    )(order, x)


def exchange(
    n, dp, scale,
    order_hbm, x_hbm, c_hbm, w_hbm, main_hbm,
    key, ig, gb, order,
    xx, cc, ck, gath, mine, give, take, part, r1, hop, zin, t3, r3, fin, main, acc,
    load_sem, send_sem, ag_recv, sib_recv, take_recv, r1_recv, z_recv, r3_recv, fin_recv,
):
    f = lax.axis_index("fsdp")
    d = lax.axis_index("dp")
    k = lax.rem(d, 2)
    sib = d + 1 - 2 * k
    chunk, key_width = main_hbm.shape
    half = key_width // 2
    depth = n // 4
    z = lax.div(f, 4)
    low = lax.rem(f, 4)
    bit0 = lax.rem(low, 2)
    bit1 = lax.div(low, 2)
    flip0 = low + 1 - 2 * bit0
    flip1 = low + 2 - 4 * bit1
    low_a = flip0 + k * (flip1 - flip0)
    low_b = flip1 + k * (flip0 - flip1)
    low_ab = 3 - low
    upper = lax.div(2 * z, depth)
    has_up = z < depth - 1
    has_dn = z > 0
    mid = jnp.logical_and(has_up, has_dn)

    def close(i):
        up = i + jnp.where(i >= z, 1, 0)
        dn = depth - 1 - i - jnp.where(depth - 1 - i <= z, 1, 0)
        return (1 - upper) * up + upper * dn

    def far(t):
        return close(depth - 2 - t) if t < depth - 1 else z

    def dev(fi, di):
        return {"fsdp": fi, "dp": di}

    to_a = dev(z * 4 + low_a, d)
    to_b = dev(z * 4 + low_b, d)
    to_sib = dev(f, sib)

    def level(zi):
        return dev(lax.rem(zi + depth, depth) * 4 + low, d)

    loads = []

    def load(src, dst):
        cp = pltpu.make_async_copy(src, dst, load_sem.at[len(loads)])
        cp.start()
        loads.append(cp)

    load(w_hbm.at[:, pl.ds(0, half)], gath.at[0, f])
    load(w_hbm.at[:, pl.ds(half, half)], gath.at[1, f])
    load(order_hbm, order)
    load(c_hbm, cc)
    for j in range(n):
        load(x_hbm.at[:, pl.ds(j * chunk, chunk)], xx.at[j])
    load(main_hbm, main)
    load_x = loads[4 : 4 + n]

    barrier = pltpu.get_barrier_semaphore()

    def greet(to):
        pl.semaphore_signal(barrier, inc=1, device_id=to, device_id_type=MESH)

    greet(to_a)
    greet(to_b)
    for s in range(1, dp):
        greet(dev(f, lax.rem(d + s, dp)))

    @pl.when(has_up)
    def _():
        greet(level(z + 1))

    @pl.when(has_dn)
    def _():
        greet(level(z - 1))

    pl.semaphore_wait(barrier, dp + 1 + jnp.where(has_up, 1, 0) + jnp.where(has_dn, 1, 0))

    sent = []

    def send(src, dst, rsem, to, cond=None):
        cp = pltpu.make_async_remote_copy(
            src_ref=src, dst_ref=dst, send_sem=send_sem, recv_sem=rsem, device_id=to, device_id_type=MESH
        )
        if cond is None:
            cp.start()
        else:
            pl.when(cond)(cp.start)
        return cp, cond

    def post(*args):
        sent.append(send(*args))

    def arrived(dst, rsem):
        pltpu.make_async_remote_copy(
            src_ref=dst, dst_ref=dst, send_sem=send_sem, recv_sem=rsem, device_id=to_sib, device_id_type=MESH
        ).wait_recv()

    def block(fb):
        return gath.at[k, fb]

    def forward(fb, to, cond=None):
        send(block(fb), block(fb), ag_recv.at[fb], to, cond)

    def forward_sib(fb):
        send(block(fb), block(fb), sib_recv.at[fb], to_sib)

    contract_rows = (((0,), (0,)), ((), ()))
    contract_cols = (((1,), (1,)), ((), ()))

    def partial(lo, t):
        fb = far(t) * 4 + lo
        prod = lax.dot_general(xx[order[fb]], ck[...], contract_rows, preferred_element_type=F32)
        give[fb] = prod[:, half:].astype(BF16)
        send(give.at[fb], take.at[fb], take_recv.at[fb], to_sib)
        mine[fb] = prod[:, :half]

    def pair(fb):
        return mine[fb] + take[fb].astype(F32)

    def across(j, t):
        zz = far(t)
        fb = zz * 4 + (low_ab if j else low_b)
        arrived(take.at[fb], take_recv.at[fb])
        part[fb] = pair(fb).astype(BF16)
        send(part.at[fb], r1.at[j, zz], r1_recv.at[j, zz], to_b)

    def from_a():
        fb = z * 4 + low_a
        arrived(block(fb), ag_recv.at[fb])
        forward(fb, level(z + 1), has_up)
        forward(fb, level(z - 1), has_dn)
        forward_sib(fb)

    def from_z(i, j):
        zz = close(i)
        fb = zz * 4 + (low_a if j else low)
        arrived(block(fb), ag_recv.at[fb])
        below = zz < z
        on = jnp.logical_or(jnp.logical_and(below, has_up), jnp.logical_and(zz > z, has_dn))
        forward(fb, level(z + jnp.where(below, 1, -1)), on)
        forward(fb, to_b)
        forward_sib(fb)

    def from_b(zz, j):
        fb = zz * 4 + (low_ab if j else low_b)
        arrived(block(fb), ag_recv.at[fb])
        forward_sib(fb)

    def ready(j, zz):
        fb = zz * 4 + (low_a if j else low)
        arrived(take.at[fb], take_recv.at[fb])
        arrived(r1.at[j, zz], r1_recv.at[j, zz])
        return pair(fb) + r1[j, zz].astype(F32)

    def along(t, j):
        zz = far(t)
        side = jnp.where(zz > z, 0, 1)
        edge = jnp.where(zz > z, z == 0, z == depth - 1)

        @pl.when(jnp.logical_not(edge))
        def _():
            arrived(zin.at[side, zz, j], z_recv.at[side, zz, j])

        total = ready(j, zz) + zin[side, zz, j].astype(F32)
        hop[j, zz] = total.astype(BF16)
        send(hop.at[j, zz], zin.at[side, zz, j], z_recv.at[side, zz, j], level(z + 1 - 2 * side))

    def settle(j):
        total = ready(j, z)

        @pl.when(has_dn)
        def _():
            arrived(zin.at[0, z, j], z_recv.at[0, z, j])

        @pl.when(has_up)
        def _():
            arrived(zin.at[1, z, j], z_recv.at[1, z, j])

        return total + zin[0, z, j].astype(F32) + zin[1, z, j].astype(F32)

    def use(fb, first=False):
        w0 = gath[0, fb]
        w1 = gath[1, fb]
        prod = lax.dot_general(cc[:, :half], w0, contract_cols, preferred_element_type=F32)
        prod = prod + lax.dot_general(cc[:, half:], w1, contract_cols, preferred_element_type=F32)
        ig[fb] = prod.astype(BF16)
        xb = xx[order[fb]]
        k0 = jnp.dot(xb, w0, preferred_element_type=F32)
        k1 = jnp.dot(xb, w1, preferred_element_type=F32)
        if first:
            acc[:, :half] = k0
            acc[:, half:] = k1
        else:
            acc[:, :half] += k0
            acc[:, half:] += k1

    def use_when(zz, lo):
        fb = zz * 4 + lo
        arrived(gath.at[1 - k, fb], sib_recv.at[fb])
        use(fb)

    loads[0].wait()
    loads[1].wait()
    forward(f, to_a)
    forward(f, level(z + 1), has_up)
    forward(f, level(z - 1), has_dn)

    @pl.when(z == 0)
    def _():
        zin[0] = jnp.zeros(zin.shape[1:], BF16)

    @pl.when(z == depth - 1)
    def _():
        zin[1] = jnp.zeros(zin.shape[1:], BF16)

    loads[3].wait()
    ck[:, :half] = cc[:, pl.ds(pl.multiple_of(k * half, half), half)]
    ck[:, half:] = cc[:, pl.ds(pl.multiple_of((1 - k) * half, half), half)]
    loads[2].wait()
    for cp in load_x:
        cp.wait()

    def start(*kinds):
        for kind, t in kinds:
            if kind == "p":
                partial(low_ab, t)
                partial(low_a, t)
                partial(low_b, t)
            else:
                across(1, t)
                across(0, t)

    start(("p", 0), ("p", 1), ("s", 0), ("p", 2), ("s", 1))
    from_a()
    forward(f, to_b)
    forward(z * 4 + low_a, to_b)
    start(("p", 3), ("s", 2))
    from_z(0, 0)

    @pl.when(mid)
    def _():
        from_z(1, 0)

    across(1, 3)
    across(0, 3)
    partial(low, 0)
    partial(low, 1)

    @pl.when(jnp.logical_not(mid))
    def _():
        along(0, 1)
        along(0, 0)
        partial(low, 2)
        from_z(0, 1)
        along(1, 1)
        partial(low, 3)
        use(f, True)
        from_b(z, 0)
        from_z(1, 0)
        along(1, 0)
        use_when(close(0), low)
        from_z(1, 1)
        along(2, 1)
        use_when(close(1), low)
        from_b(z, 1)
        along(2, 0)
        use_when(z, low_b)
        use_when(z, low_a)
        from_z(2, 0)
        from_b(close(0), 0)
        from_z(2, 1)

    @pl.when(mid)
    def _():
        partial(low, 2)
        from_z(0, 1)
        from_z(1, 1)
        partial(low, 3)
        use(f, True)
        from_b(z, 0)
        from_z(2, 0)
        along(0, 1)
        use_when(close(0), low)
        use_when(close(1), low)
        from_z(2, 1)
        along(0, 0)
        use_when(z, low_b)
        along(2, 1)
        from_b(z, 1)
        along(1, 1)
        use_when(z, low_a)
        along(2, 0)
        from_b(close(0), 0)
        along(1, 0)

    use_when(close(2), low)
    use_when(z, low_ab)
    t3[...] = settle(1).astype(BF16)
    send(t3, r3, r3_recv, to_a)
    from_b(close(0), 1)
    use_when(close(0), low_b)
    use_when(close(0), low_a)
    from_b(close(1), 0)
    use_when(close(0), low_ab)
    use_when(close(1), low_b)
    total = settle(0)
    from_b(close(1), 1)
    use_when(close(1), low_a)
    arrived(r3, r3_recv)
    fin[d] = total + r3[...].astype(F32)
    for s in range(1, dp):
        send(fin.at[d], fin.at[d], fin_recv.at[d], dev(f, lax.rem(d + s, dp)))
    use_when(close(1), low_ab)
    from_b(close(2), 0)
    use_when(close(2), low_b)
    from_b(close(2), 1)
    use_when(close(2), low_a)
    loads[-1].wait()
    for s in range(1, dp):
        src = lax.rem(d + s, dp)
        arrived(fin.at[src], fin_recv.at[src])
    for h in range(2):
        total = fin[h]
        for g in range(1, dp // 2):
            total = total + fin[2 * g + h]
        side = slice(h * half, (h + 1) * half)
        gb[:, side] = main[:, side] + total * scale
    use_when(close(2), low_ab)
    key[...] = acc[...].astype(BF16)

    per_z = jnp.where(has_up, z + 1, 0) + jnp.where(has_dn, depth - z, 0)
    blocks = 4 + 6 * (depth - 1) + 8 * depth + 1 + 2 * per_z

    def left(_, carry):
        send_done(give.at[f])
        return carry

    def send_done(src):
        pltpu.make_async_remote_copy(
            src_ref=src, dst_ref=src, send_sem=send_sem, recv_sem=r3_recv, device_id=to_sib, device_id_type=MESH
        ).wait_send()

    lax.fori_loop(0, blocks, left, 0)
    for s in range(1, dp):
        send_done(fin.at[d])


def place(order, key, ig, gb, key_hbm, ig_hbm, gb_hbm, sem):
    n, _, chunk = ig.shape
    puts = []
    for fb in range(n):
        there = pl.ds(pl.multiple_of(order[fb] * chunk, chunk), chunk)
        puts.append(pltpu.make_async_copy(ig.at[fb], ig_hbm.at[:, there], sem.at[fb]))
    puts.append(pltpu.make_async_copy(key, key_hbm, sem.at[n]))
    puts.append(pltpu.make_async_copy(gb, gb_hbm, sem.at[n + 1]))
    for cp in puts:
        cp.start()
    for cp in puts:
        cp.wait()


def near(x, c, w, main, order, n, dp, scale):
    rows, width = x.shape
    chunk, key_width = main.shape
    half = key_width // 2
    depth = n // 4
    dma = pltpu.SemaphoreType.DMA
    block = (chunk, half)
    hbm = pl.BlockSpec(memory_space=pltpu.HBM)
    smem = pl.BlockSpec(memory_space=pltpu.SMEM)
    vmem = pl.BlockSpec(memory_space=pltpu.VMEM)
    operands = [pltpu.with_memory_space_constraint(a, pltpu.HBM) for a in (order, x, c, w, main)]
    key, ig, gb, order = pl.pallas_call(
        functools.partial(exchange, n, dp, scale),
        out_shape=(
            pltpu.VMEM((rows, key_width), BF16),
            pltpu.VMEM((n, rows, chunk), BF16),
            pltpu.VMEM((chunk, key_width), F32),
            pltpu.SMEM((n,), jnp.int32),
        ),
        in_specs=[hbm] * 5,
        out_specs=(vmem,) * 3 + (smem,),
        scratch_shapes=[
            pltpu.VMEM((n, rows, chunk), BF16),
            pltpu.VMEM((rows, key_width), BF16),
            pltpu.VMEM((rows, key_width), BF16),
            pltpu.VMEM((2, n) + block, BF16),
            pltpu.VMEM((n,) + block, F32),
            pltpu.VMEM((n,) + block, BF16),
            pltpu.VMEM((n,) + block, BF16),
            pltpu.VMEM((n,) + block, BF16),
            pltpu.VMEM((2, depth) + block, BF16),
            pltpu.VMEM((2, depth) + block, BF16),
            pltpu.VMEM((2, depth, 2) + block, BF16),
            pltpu.VMEM(block, BF16),
            pltpu.VMEM(block, BF16),
            pltpu.VMEM((dp,) + block, F32),
            pltpu.VMEM((chunk, key_width), F32),
            pltpu.VMEM((rows, key_width), F32),
            dma((n + 5,)),
            dma,
            dma((n,)),
            dma((n,)),
            dma((n,)),
            dma((2, depth)),
            dma((2, depth, 2)),
            dma,
            dma((dp,)),
        ],
        compiler_params=pltpu.CompilerParams(
            collective_id=0, has_side_effects=True, vmem_limit_bytes=36 * 1024 * 1024
        ),
    )(*operands)
    return pl.pallas_call(
        place,
        out_shape=(
            jax.ShapeDtypeStruct((rows, key_width), BF16),
            jax.ShapeDtypeStruct((rows, width), BF16),
            jax.ShapeDtypeStruct((chunk, key_width), F32),
        ),
        in_specs=[smem] + [vmem] * 3,
        out_specs=(hbm,) * 3,
        scratch_shapes=[dma((n + 2,))],
        compiler_params=pltpu.CompilerParams(vmem_limit_bytes=8 * 1024 * 1024),
    )(order, key, ig, gb)


def body(normed, kv_cotangent, kv_weight, main_grad, owner_order):
    micro_count, tok_dev, width = normed.shape
    shard_rows, key_width = kv_weight.shape
    n = lax.axis_size("fsdp")
    dp = lax.axis_size("dp")
    rows = micro_count * tok_dev
    half = key_width // 2
    depth = n // 4
    scale = 1.0 / math.sqrt(rows * n * dp)
    chunk = shard_rows if shard_rows % 128 == 0 else max(shard_rows, 256)
    if depth == 4 and shard_rows % 128 == 0:
        key, ig, gb = near(
            normed.reshape(rows, width), kv_cotangent.reshape(rows, key_width), kv_weight, main_grad, owner_order, n, dp, scale
        )
        return (
            key.reshape(micro_count, tok_dev, key_width),
            ig.reshape(micro_count, tok_dev, width),
            gb,
        )
    x = reorder(normed.reshape(rows, width), owner_order, False)
    chunks = width // chunk
    dma = pltpu.SemaphoreType.DMA
    half_block = (shard_rows, half)
    any_spec = pl.BlockSpec(memory_space=pl.ANY)
    key, ig, gb = pl.pallas_call(
        functools.partial(kernel, n, dp, chunk, scale),
        out_shape=(
            jax.ShapeDtypeStruct((rows, key_width), BF16),
            jax.ShapeDtypeStruct((rows, width), BF16),
            jax.ShapeDtypeStruct((shard_rows, key_width), F32),
        ),
        in_specs=[any_spec] * 4,
        out_specs=(any_spec,) * 3,
        scratch_shapes=[
            pltpu.VMEM((2, rows, width), BF16),
            pltpu.VMEM((2, rows, key_width), BF16),
            pltpu.VMEM((2 * rows, half), BF16),
            pltpu.VMEM((2, n) + half_block, BF16),
            pltpu.VMEM((n,) + half_block, BF16),
            pltpu.VMEM((2, depth) + half_block, BF16),
            pltpu.VMEM((depth,) + half_block, BF16),
            pltpu.VMEM((depth,) + half_block, BF16),
            pltpu.VMEM((depth,) + half_block, BF16),
            pltpu.VMEM((depth,) + half_block, BF16),
            pltpu.VMEM((dp,) + half_block, F32),
            pltpu.VMEM((shard_rows, key_width), F32),
            pltpu.VMEM((shard_rows, key_width), F32),
            pltpu.VMEM((rows, key_width), BF16),
            pltpu.VMEM((rows, width), BF16),
            pltpu.VMEM((rows, key_width), F32),
            dma((5,)),
            dma((chunks + 2,)),
            dma,
            dma((2,)),
            dma((depth,)),
            dma((depth,)),
            dma((2 * depth,)),
            dma((n,)),
            dma((2, depth)),
            dma((depth,)),
            dma((depth,)),
            dma((dp,)),
        ],
        compiler_params=pltpu.CompilerParams(
            collective_id=0, has_side_effects=True
        ),
    )(x, kv_cotangent.reshape(rows, key_width), kv_weight, main_grad)
    ig = reorder(ig, owner_order, True)
    return (
        key.reshape(micro_count, tok_dev, key_width),
        ig.reshape(micro_count, tok_dev, width),
        gb,
    )


def solution(mesh):
    in_specs = (
        P(None, ("fsdp", "dp"), None),
        P(None, ("fsdp", "dp"), None),
        P("fsdp", None),
        P("fsdp", None),
        P(),
    )
    out_specs = (P(None, ("fsdp", "dp"), None), P(None, ("fsdp", "dp"), None), P("fsdp", None))
    return jax.shard_map(body, mesh=mesh, in_specs=in_specs, out_specs=out_specs, check_vma=False)
```

```python
import functools
import math

import jax
import jax.numpy as jnp
from jax import lax
from jax.experimental import pallas as pl
from jax.experimental.pallas import tpu as pltpu
from jax.sharding import PartitionSpec as P

MESH = pl.DeviceIdType.MESH
F32 = jnp.float32
BF16 = jnp.bfloat16
SLOT = (0, 1, 1, 2)
SWAP = (0, 2, 1, 3)


def kernel(
    n, dp, chunk, scale,
    x_hbm, c_hbm, w_hbm, main_hbm,
    key_hbm, ig_hbm, gb_hbm,
    xx, cc, ck, gath, part, r1, t1, r2, t2, r3, fin, main, gb, key, ig, acc,
    load_sem, out_sem, send_sem, x_recv, az_recv, a1_recv, a2_recv, ad_recv, r1_recv, r2_recv, r3_recv, rd_recv,
):
    f = lax.axis_index("fsdp")
    d = lax.axis_index("dp")
    k = lax.rem(d, 2)
    sib = d + 1 - 2 * k
    rows, width = x_hbm.shape
    key_width = c_hbm.shape[1]
    half = key_width // 2
    depth = n // 4
    chunks = width // chunk
    z = lax.div(f, 4)
    low = lax.rem(f, 4)
    bit0 = lax.rem(low, 2)
    bit1 = lax.div(low, 2)
    flip_x = low + 1 - 2 * bit0
    flip_y = low + 2 - 4 * bit1
    low1 = flip_x + k * (flip_y - flip_x)
    low2 = flip_y + k * (flip_x - flip_y)
    low12 = 3 - low
    p1 = z * 4 + low1
    p2 = z * 4 + low2
    steps = sorted(range(1, depth), key=lambda s: (min(s, depth - s), s))

    def peer(s):
        return lax.rem(z + s, depth)

    def dev(fi, di):
        return {"fsdp": fi, "dp": di}

    loads = []

    def load(src, dst, i):
        cp = pltpu.make_async_copy(src, dst, load_sem.at[i])
        cp.start()
        loads.append(cp)

    load(w_hbm.at[:, pl.ds(0, half)], gath.at[0, f], 0)
    load(w_hbm.at[:, pl.ds(half, half)], gath.at[1, f], 1)
    load(c_hbm, cc.at[0], 2)
    load(x_hbm, xx.at[0], 3)
    load(main_hbm, main, 4)

    barrier = pltpu.get_barrier_semaphore()
    greeted = [dev(peer(s) * 4 + low, d) for s in steps]
    greeted += [dev(p1, d), dev(p2, d)]
    greeted += [dev(f, lax.rem(d + s, dp)) for s in range(1, dp)]
    for g in greeted:
        pl.semaphore_signal(barrier, inc=1, device_id=g, device_id_type=MESH)
    pl.semaphore_wait(barrier, len(greeted))

    sent = []

    def send(src, dst, rsem, to):
        cp = pltpu.make_async_remote_copy(
            src_ref=src, dst_ref=dst, send_sem=send_sem, recv_sem=rsem, device_id=to, device_id_type=MESH
        )
        cp.start()
        sent.append(cp)

    def arrived(dst, rsem, frm):
        pltpu.make_async_remote_copy(
            src_ref=dst, dst_ref=dst, send_sem=send_sem, recv_sem=rsem, device_id=frm, device_id_type=MESH
        ).wait_recv()

    to_sib = dev(f, sib)
    to1 = dev(p1, d)
    to2 = dev(p2, d)

    send(x_hbm, xx.at[1], x_recv.at[0], to_sib)
    send(c_hbm, cc.at[1], x_recv.at[1], to_sib)
    loads[0].wait()
    loads[1].wait()

    def block(fi):
        return gath.at[k, fi]

    send(block(f), block(f), a1_recv.at[z], to1)
    send(block(f), block(f), a2_recv.at[z], to2)
    for s in steps:
        send(block(f), block(f), az_recv.at[z], dev(peer(s) * 4 + low, d))

    loads[2].wait()
    loads[3].wait()
    arrived(cc.at[1], x_recv.at[1], to_sib)
    arrived(xx.at[1], x_recv.at[0], to_sib)
    side = pl.ds(pl.multiple_of(k * half, half), half)
    ck[...] = cc[:, :, side].reshape(2 * rows, half)

    per = chunk // part.shape[1]
    ring = steps + [0]
    blockwise = per == 1

    def partial(cols):
        both = xx[:, :, cols].reshape(2 * rows, chunk)
        prod = lax.dot_general(both, ck[...], (((0,), (0,)), ((), ())), preferred_element_type=F32)
        return prod.astype(BF16)

    def feature_block(fb):
        return pl.ds(pl.multiple_of(fb * chunk, chunk), chunk)

    def partials(lo):
        if blockwise:
            for s in ring:
                fb = peer(s) * 4 + lo
                part[fb] = partial(feature_block(fb))
                if lo is low12:
                    send(part.at[fb], r1.at[0, peer(s)], r1_recv.at[0, peer(s)], to1)
                if lo is low1:
                    send(part.at[fb], r1.at[1, peer(s)], r1_recv.at[1, peer(s)], to1)

    if not blockwise:
        for j in range(chunks):
            made = partial(pl.ds(j * chunk, chunk))
            part[j * per : (j + 1) * per] = made.reshape(per, part.shape[1], half)
        for s in ring:
            send(part.at[peer(s) * 4 + low12], r1.at[0, peer(s)], r1_recv.at[0, peer(s)], to1)
    partials(low12)
    for s in steps:
        zb = peer(s)
        fb = zb * 4 + low
        arrived(block(fb), az_recv.at[zb], dev(fb, d))
        send(block(fb), block(fb), a1_recv.at[zb], to1)
        send(block(fb), block(fb), a2_recv.at[zb], to2)
        send(block(fb), block(fb), ad_recv.at[fb], to_sib)
    if not blockwise:
        for s in ring:
            send(part.at[peer(s) * 4 + low1], r1.at[1, peer(s)], r1_recv.at[1, peer(s)], to1)
    partials(low1)
    partials(low2)
    partials(low)

    outs = []

    def put(src, dst, i):
        cp = pltpu.make_async_copy(src, dst, out_sem.at[i])
        cp.start()
        outs.append(cp)

    contract = (((1,), (1,)), ((), ()))

    def from_sib(lo):
        for s in [0] + steps:
            fb = peer(s) * 4 + lo
            if s or lo is not low:
                arrived(gath.at[1 - k, fb], ad_recv.at[fb], to_sib)

    def use(lo):
        if not blockwise:
            return
        from_sib(lo)
        for s in [0] + steps:
            fb = peer(s) * 4 + lo
            cols = feature_block(fb)
            w0 = gath[0, fb]
            w1 = gath[1, fb]
            prod = lax.dot_general(cc[0, :, :half], w0, contract, preferred_element_type=F32)
            prod = prod + lax.dot_general(cc[0, :, half:], w1, contract, preferred_element_type=F32)
            ig[:, cols] = prod.astype(BF16)
            put(ig.at[:, cols], ig_hbm.at[:, cols], len(outs))
            xb = xx[0, :, cols]
            k0 = jnp.dot(xb, w0, preferred_element_type=F32)
            k1 = jnp.dot(xb, w1, preferred_element_type=F32)
            if s == 0 and lo is low:
                acc[:, :half] = k0
                acc[:, half:] = k1
            else:
                acc[:, :half] += k0
                acc[:, half:] += k1

    for s in [0] + steps:
        zb = peer(s)
        fb = zb * 4 + low1
        arrived(block(fb), a1_recv.at[zb], to1)
        send(block(fb), block(fb), a2_recv.at[depth + zb], to2)
        send(block(fb), block(fb), ad_recv.at[fb], to_sib)
    for s in ring:
        zb = peer(s)
        arrived(r1.at[0, zb], r1_recv.at[0, zb], to1)
        t1[zb] = (part[zb * 4 + low2].astype(F32) + r1[0, zb].astype(F32)).astype(BF16)
        send(t1.at[zb], r2.at[zb], r2_recv.at[zb], to2)
    use(low)
    for s in steps:
        zb = peer(s)
        arrived(r1.at[1, zb], r1_recv.at[1, zb], to1)
        arrived(r2.at[zb], r2_recv.at[zb], to2)
        t2[zb] = (part[zb * 4 + low].astype(F32) + r1[1, zb].astype(F32) + r2[zb].astype(F32)).astype(BF16)
        send(t2.at[zb], r3.at[z], r3_recv.at[z], dev(zb * 4 + low, d))
    for s in [0] + steps:
        zb = peer(s)
        fb = zb * 4 + low2
        arrived(block(fb), a2_recv.at[zb], to2)
        send(block(fb), block(fb), ad_recv.at[fb], to_sib)
    use(low1)
    use(low2)
    for s in [0] + steps:
        zb = peer(s)
        fb = zb * 4 + low12
        arrived(block(fb), a2_recv.at[depth + zb], to2)
        send(block(fb), block(fb), ad_recv.at[fb], to_sib)

    arrived(r1.at[1, z], r1_recv.at[1, z], to1)
    arrived(r2.at[z], r2_recv.at[z], to2)
    total = part[f].astype(F32) + r1[1, z].astype(F32) + r2[z].astype(F32)
    for s in steps:
        arrived(r3.at[peer(s)], r3_recv.at[peer(s)], dev(peer(s) * 4 + low, d))
        total = total + r3[peer(s)].astype(F32)
    fin[d] = total
    for s in range(1, dp):
        send(fin.at[d], fin.at[d], rd_recv.at[d], dev(f, lax.rem(d + s, dp)))

    use(low12)
    if blockwise:
        key[...] = acc[...].astype(BF16)
    else:
        for lo in (low, low1, low2, low12):
            from_sib(lo)
        for j in range(chunks):
            w0 = gath[0, j * per : (j + 1) * per].reshape(chunk, half)
            w1 = gath[1, j * per : (j + 1) * per].reshape(chunk, half)
            prod = lax.dot_general(cc[0, :, :half], w0, contract, preferred_element_type=F32)
            prod = prod + lax.dot_general(cc[0, :, half:], w1, contract, preferred_element_type=F32)
            ig[:, j * chunk : (j + 1) * chunk] = prod.astype(BF16)
        put(ig, ig_hbm, 0)
        for h in range(2):
            w = gath[h].reshape(width, half)
            key[:, h * half : (h + 1) * half] = jnp.dot(xx[0], w, preferred_element_type=F32).astype(BF16)
    put(key, key_hbm, len(outs))

    for s in range(1, dp):
        src = lax.rem(d + s, dp)
        arrived(fin.at[src], rd_recv.at[src], dev(f, src))
    loads[4].wait()
    for h in range(2):
        total = fin[h]
        for g in range(1, dp // 2):
            total = total + fin[2 * g + h]
        cols = slice(h * half, (h + 1) * half)
        gb[:, cols] = main[:, cols] + total * scale
    put(gb, gb_hbm, len(outs))
    for cp in sent:
        cp.wait_send()
    for cp in outs:
        cp.wait()


def reorder_kernel(depth, scatter, order_ref, x_ref, y_ref):
    for j in range(x_ref.shape[1] // depth):
        here = slice(j * depth, (j + 1) * depth)
        there = pl.ds(pl.multiple_of(order_ref[j] * depth, depth), depth)
        if scatter:
            y_ref[:, there] = x_ref[:, here]
        else:
            y_ref[:, here] = x_ref[:, there]


def reorder(x, order, scatter):
    rows, width = x.shape
    n = order.shape[0]
    depth = width // n
    if depth % 128:
        if scatter:
            order = jnp.argsort(order)
        return jnp.take(x.reshape(rows, n, depth), order, axis=1, mode="clip").reshape(rows, width)
    tile = rows // 4
    spec = pl.BlockSpec((tile, width), lambda i: (i, 0))
    return pl.pallas_call(
        functools.partial(reorder_kernel, depth, scatter),
        grid=(rows // tile,),
        out_shape=jax.ShapeDtypeStruct((rows, width), x.dtype),
        in_specs=[pl.BlockSpec(memory_space=pltpu.SMEM), spec],
        out_specs=spec,
        cost_estimate=pl.CostEstimate(flops=0, bytes_accessed=4 * rows * width, transcendentals=0),
    )(order, x)


def exchange(
    n, dp, scale,
    order_hbm, x_hbm, c_hbm, w_hbm, main_hbm,
    key, ig, gb, order,
    xx, cc, ck, gath, mine, give, take, part, r1, hop, zin, t3, r3, fin, main, acc,
    load_sem, send_sem, ag_recv, b_recv, sib_recv, take_recv, r1_recv, z_recv, r3_recv, fin_recv,
):
    f = lax.axis_index("fsdp")
    d = lax.axis_index("dp")
    k = lax.rem(d, 2)
    sib = d + 1 - 2 * k
    chunk, key_width = main_hbm.shape
    half = key_width // 2
    part_rows = chunk // 2
    depth = n // 4
    z = lax.div(f, 4)
    low = lax.rem(f, 4)
    bit0 = lax.rem(low, 2)
    bit1 = lax.div(low, 2)
    flip0 = low + 1 - 2 * bit0
    flip1 = low + 2 - 4 * bit1
    low_a = flip0 + k * (flip1 - flip0)
    low_b = flip1 + k * (flip0 - flip1)
    low_ab = 3 - low
    lows = (low, low_a, low_b, low_ab)
    upper = lax.div(2 * z, depth)
    has_up = z < depth - 1
    has_dn = z > 0
    mid = jnp.logical_and(has_up, has_dn)

    def close(i):
        up = i + jnp.where(i >= z, 1, 0)
        dn = depth - 1 - i - jnp.where(depth - 1 - i <= z, 1, 0)
        return (1 - upper) * up + upper * dn

    def far(t):
        return close(depth - 2 - t) if t < depth - 1 else z

    def dev(fi, di):
        return {"fsdp": fi, "dp": di}

    to_a = dev(z * 4 + low_a, d)
    to_b = dev(z * 4 + low_b, d)
    to_sib = dev(f, sib)

    def level(zi):
        return dev(lax.rem(zi + depth, depth) * 4 + low, d)

    loads = []

    def load(src, dst):
        cp = pltpu.make_async_copy(src, dst, load_sem.at[len(loads)])
        cp.start()
        loads.append(cp)

    def loaded(*span):
        for cp in loads[slice(*span)]:
            cp.wait()

    load(w_hbm.at[:, pl.ds(0, half)], gath.at[0, z, 0])
    load(w_hbm.at[:, pl.ds(half, half)], gath.at[1, z, 0])
    load(order_hbm, order)
    load(c_hbm, cc)
    for j in range(n):
        load(x_hbm.at[:, pl.ds(j * chunk, chunk)], xx.at[j])
    load(main_hbm, main)

    barrier = pltpu.get_barrier_semaphore()

    def greet(to):
        pl.semaphore_signal(barrier, inc=1, device_id=to, device_id_type=MESH)

    greet(to_a)
    greet(to_b)
    for s in range(1, dp):
        greet(dev(f, lax.rem(d + s, dp)))

    @pl.when(has_up)
    def _():
        greet(level(z + 1))

    @pl.when(has_dn)
    def _():
        greet(level(z - 1))

    pl.semaphore_wait(barrier, dp + 1 + jnp.where(has_up, 1, 0) + jnp.where(has_dn, 1, 0))

    sent = []

    def send(src, dst, rsem, to, cond=None):
        cp = pltpu.make_async_remote_copy(
            src_ref=src, dst_ref=dst, send_sem=send_sem, recv_sem=rsem, device_id=to, device_id_type=MESH
        )
        if cond is None:
            cp.start()
        else:
            pl.when(cond)(cp.start)
        return cp, cond

    def post(*args):
        sent.append(send(*args))

    def arrived(dst, rsem):
        pltpu.make_async_remote_copy(
            src_ref=dst, dst_ref=dst, send_sem=send_sem, recv_sem=rsem, device_id=to_sib, device_id_type=MESH
        ).wait_recv()

    def rows_of(p):
        return pl.ds(p * part_rows, part_rows)

    def forward(zz, kind):
        send(gath.at[k, zz, kind], gath.at[k, zz, kind + 2], b_recv.at[kind, zz], to_b)

    def forward_piece(zz, kind, there, p, to, cond=None):
        src = gath.at[k, zz, kind, rows_of(p)]
        dst = gath.at[k, zz, there, rows_of(p)]
        send(src, dst, ag_recv.at[there, zz, p], to, cond)

    def forward_sib(zz, kind):
        send(gath.at[k, zz, kind], gath.at[k, zz, SWAP[kind]], sib_recv.at[SLOT[kind], zz], to_sib)

    contract_rows = (((0,), (0,)), ((), ()))
    contract_cols = (((1,), (1,)), ((), ()))

    def partial(kind, t):
        zz = far(t)
        prod = lax.dot_general(xx[order[zz * 4 + lows[kind]]], ck[...], contract_rows, preferred_element_type=F32)
        give[zz, kind] = prod[:, half:].astype(BF16)
        there = 3 - SWAP[kind]
        send(give.at[zz, kind], take.at[zz, there], take_recv.at[there // 2, zz], to_sib)
        mine[zz, kind] = prod[:, :half]

    def taken(group, zz):
        arrived(take.at[zz, pl.ds(2 * group, 2)], take_recv.at[group, zz])

    def pair(zz, kind, span):
        return mine[zz, kind, span] + take[zz, 3 - kind, span].astype(F32)

    def across(j, t):
        zz = far(t)
        if j:
            taken(0, zz)
        part[j, zz] = pair(zz, 2 + j, slice(None)).astype(BF16)
        send(part.at[j, zz], r1.at[j, zz], r1_recv.at[j, zz], to_b)

    def from_a(p):
        arrived(gath.at[k, z, 1, rows_of(p)], ag_recv.at[1, z, p])
        forward_piece(z, 1, 1, p, level(z + 1), has_up)
        forward_piece(z, 1, 1, p, level(z - 1), has_dn)
        if p:
            forward(z, 1)
            forward_sib(z, 1)

    def from_z(i, j, p):
        zz = close(i)
        arrived(gath.at[k, zz, j, rows_of(p)], ag_recv.at[j, zz, p])
        below = zz < z
        on = jnp.logical_or(jnp.logical_and(below, has_up), jnp.logical_and(zz > z, has_dn))
        forward_piece(zz, j, j, p, level(z + jnp.where(below, 1, -1)), on)
        if p:
            forward(zz, j)
            forward_sib(zz, j)

    def from_b(zz, j):
        arrived(gath.at[k, zz, 2 + j], b_recv.at[j, zz])
        forward_sib(zz, 2 + j)

    def ready(j, zz):
        if j:
            taken(1, zz)
        arrived(r1.at[j, zz], r1_recv.at[j, zz])

    def summed(j, zz, span):
        return pair(zz, j, span) + r1[j, zz, span].astype(F32)

    def along(t, j, p):
        zz = far(t)
        side = jnp.where(zz > z, 0, 1)
        edge = jnp.where(zz > z, z == 0, z == depth - 1)
        span = rows_of(p)
        spot = zin.at[side, zz, j, span]
        if not p:
            ready(j, zz)

        @pl.when(jnp.logical_not(edge))
        def _():
            arrived(spot, z_recv.at[zz, j, p])

        total = summed(j, zz, span) + spot[...].astype(F32)
        hop[j, zz, span] = total.astype(BF16)
        there = z + 1 - 2 * side
        slot = jnp.where(side * depth + zz == depth + there, depth, zz)
        send(hop.at[j, zz, span], spot, z_recv.at[slot, j, p], level(there))

    def settle(j, p):
        span = rows_of(p)
        if not p:
            ready(j, z)

        @pl.when(has_dn)
        def _():
            arrived(zin.at[0, z, j, span], z_recv.at[z, j, p])

        @pl.when(has_up)
        def _():
            arrived(zin.at[1, z, j, span], z_recv.at[depth, j, p])

        return summed(j, z, span) + zin[0, z, j, span].astype(F32) + zin[1, z, j, span].astype(F32)

    def use(zz, kind, first=False):
        fb = zz * 4 + lows[kind]
        w0 = gath[0, zz, kind]
        w1 = gath[1, zz, kind]
        prod = lax.dot_general(cc[:, :half], w0, contract_cols, preferred_element_type=F32)
        prod = prod + lax.dot_general(cc[:, half:], w1, contract_cols, preferred_element_type=F32)
        ig[fb] = prod.astype(BF16)
        xb = xx[order[fb]]
        k0 = jnp.dot(xb, w0, preferred_element_type=F32)
        k1 = jnp.dot(xb, w1, preferred_element_type=F32)
        if first:
            acc[:, :half] = k0
            acc[:, half:] = k1
        else:
            acc[:, :half] += k0
            acc[:, half:] += k1

    def use_when(zz, *kinds):
        arrived(gath.at[1 - k, zz, pl.ds(kinds[0], len(kinds))], sib_recv.at[SLOT[kinds[0]], zz])
        for kind in kinds:
            use(zz, kind)

    loaded(0, 2)
    for p in range(2):
        forward_piece(z, 0, 1, p, to_a)
        forward_piece(z, 0, 0, p, level(z + 1), has_up)
        forward_piece(z, 0, 0, p, level(z - 1), has_dn)

    @pl.when(z == 0)
    def _():
        zin[0] = jnp.zeros(zin.shape[1:], BF16)

    @pl.when(z == depth - 1)
    def _():
        zin[1] = jnp.zeros(zin.shape[1:], BF16)

    loaded(2, -1)
    ck[:, :half] = cc[:, pl.ds(pl.multiple_of(k * half, half), half)]
    ck[:, half:] = cc[:, pl.ds(pl.multiple_of((1 - k) * half, half), half)]
    def start(*tasks):
        for what, t in tasks:
            if what == "p":
                partial(3, t)
                partial(1, t)
                partial(2, t)
            else:
                across(1, t)
                across(0, t)

    start(("p", 0))
    partial(3, 1)
    forward(z, 0)
    partial(1, 1)
    partial(2, 1)
    start(("s", 0), ("p", 2))
    from_a(0)
    start(("s", 1))
    from_a(1)
    start(("p", 3), ("s", 2))
    for p in range(2):
        from_z(0, 0, p)

        @pl.when(mid)
        def _():
            from_z(1, 0, p)

    start(("s", 3))
    partial(0, 0)
    partial(0, 1)

    def both(fn, *args):
        fn(*args, 0)
        fn(*args, 1)

    @pl.when(jnp.logical_not(mid))
    def _():
        both(along, 0, 1)
        partial(0, 2)
        both(along, 0, 0)
        both(from_z, 0, 1)
        both(along, 1, 1)
        partial(0, 3)
        use(z, 0, True)
        both(along, 1, 0)
        both(from_z, 1, 0)
        from_b(z, 0)
        use_when(close(0), 0)
        from_z(1, 1, 0)
        both(along, 2, 1)
        from_z(1, 1, 1)
        both(along, 2, 0)
        use_when(close(1), 0)
        both(from_z, 2, 0)
        from_b(z, 1)
        use_when(z, 1, 2)
        from_b(close(0), 0)
        both(from_z, 2, 1)

    @pl.when(mid)
    def _():
        partial(0, 2)
        from_z(0, 1, 0)
        from_z(1, 1, 0)
        from_z(0, 1, 1)
        from_z(1, 1, 1)
        partial(0, 3)
        use(z, 0, True)
        both(from_z, 2, 0)
        both(along, 0, 1)
        from_b(z, 0)
        use_when(close(0), 0)
        along(0, 0, 0)
        from_z(2, 1, 0)
        along(0, 0, 1)
        from_z(2, 1, 1)
        use_when(close(1), 0)
        both(along, 2, 1)
        both(along, 1, 1)
        from_b(z, 1)
        both(along, 2, 0)
        use_when(z, 1, 2)
        from_b(close(0), 0)
        both(along, 1, 0)

    use_when(close(2), 0)
    use_when(z, 3)
    for p in range(2):
        t3[rows_of(p)] = settle(1, p).astype(BF16)
        send(t3.at[rows_of(p)], r3.at[rows_of(p)], r3_recv.at[p], to_a)
    from_b(close(0), 1)
    use_when(close(0), 1, 2)
    from_b(close(1), 0)
    use_when(close(0), 3)
    from_b(close(1), 1)
    use_when(close(1), 1, 2)
    from_b(close(2), 0)
    use_when(close(1), 3)
    for p in range(2):
        fin[d, rows_of(p)] = settle(0, p)
    for p in range(2):
        arrived(r3.at[rows_of(p)], r3_recv.at[p])
        fin[d, rows_of(p)] += r3[rows_of(p)].astype(F32)
    for s in range(1, dp):
        send(fin.at[d], fin.at[d], fin_recv.at[d], dev(f, lax.rem(d + s, dp)))
    from_b(close(2), 1)
    use_when(close(2), 1, 2)
    loaded(-1, None)
    for s in range(1, dp):
        src = lax.rem(d + s, dp)
        arrived(fin.at[src], fin_recv.at[src])
    for h in range(2):
        total = fin[h]
        for g in range(1, dp // 2):
            total = total + fin[2 * g + h]
        side = slice(h * half, (h + 1) * half)
        gb[:, side] = main[:, side] + total * scale
    use_when(close(2), 3)
    key[...] = acc[...].astype(BF16)

    def send_done(src):
        pltpu.make_async_remote_copy(
            src_ref=src, dst_ref=src, send_sem=send_sem, recv_sem=r3_recv.at[0], device_id=to_sib, device_id_type=MESH
        ).wait_send()

    def left(_, carry):
        send_done(give.at[0, 0])
        return carry

    blocks = 4 + 6 * (depth - 1) + 8 * depth + 1
    for _ in range(blocks // n):
        send_done(give)
    per_z = jnp.where(has_up, z + 1, 0) + jnp.where(has_dn, depth - z, 0)
    lax.fori_loop(0, blocks % n + 2 * per_z, left, 0)
    for s in range(1, dp):
        send_done(fin.at[d])


def place(order, key, ig, gb, key_hbm, ig_hbm, gb_hbm, sem):
    n, _, chunk = ig.shape
    puts = []
    for fb in range(n):
        there = pl.ds(pl.multiple_of(order[fb] * chunk, chunk), chunk)
        puts.append(pltpu.make_async_copy(ig.at[fb], ig_hbm.at[:, there], sem.at[fb]))
    puts.append(pltpu.make_async_copy(key, key_hbm, sem.at[n]))
    puts.append(pltpu.make_async_copy(gb, gb_hbm, sem.at[n + 1]))
    for cp in puts:
        cp.start()
    for cp in puts:
        cp.wait()


def near(x, c, w, main, order, n, dp, scale):
    rows, width = x.shape
    chunk, key_width = main.shape
    half = key_width // 2
    depth = n // 4
    dma = pltpu.SemaphoreType.DMA
    block = (chunk, half)
    hbm = pl.BlockSpec(memory_space=pltpu.HBM)
    smem = pl.BlockSpec(memory_space=pltpu.SMEM)
    vmem = pl.BlockSpec(memory_space=pltpu.VMEM)
    operands = [pltpu.with_memory_space_constraint(a, pltpu.HBM) for a in (order, x, c, w, main)]
    key, ig, gb, order = pl.pallas_call(
        functools.partial(exchange, n, dp, scale),
        out_shape=(
            pltpu.VMEM((rows, key_width), BF16),
            pltpu.VMEM((n, rows, chunk), BF16),
            pltpu.VMEM((chunk, key_width), F32),
            pltpu.SMEM((n,), jnp.int32),
        ),
        in_specs=[hbm] * 5,
        out_specs=(vmem,) * 3 + (smem,),
        scratch_shapes=[
            pltpu.VMEM((n, rows, chunk), BF16),
            pltpu.VMEM((rows, key_width), BF16),
            pltpu.VMEM((rows, key_width), BF16),
            pltpu.VMEM((2, depth, 4) + block, BF16),
            pltpu.VMEM((depth, 4) + block, F32),
            pltpu.VMEM((depth, 4) + block, BF16),
            pltpu.VMEM((depth, 4) + block, BF16),
            pltpu.VMEM((2, depth) + block, BF16),
            pltpu.VMEM((2, depth) + block, BF16),
            pltpu.VMEM((2, depth) + block, BF16),
            pltpu.VMEM((2, depth, 2) + block, BF16),
            pltpu.VMEM(block, BF16),
            pltpu.VMEM(block, BF16),
            pltpu.VMEM((dp,) + block, F32),
            pltpu.VMEM((chunk, key_width), F32),
            pltpu.VMEM((rows, key_width), F32),
            dma((n + 5,)),
            dma,
            dma((2, depth, 2)),
            dma((2, depth)),
            dma((3, depth)),
            dma((2, depth)),
            dma((2, depth)),
            dma((depth + 1, 2, 2)),
            dma((2,)),
            dma((dp,)),
        ],
        compiler_params=pltpu.CompilerParams(
            collective_id=0, has_side_effects=True, vmem_limit_bytes=36 * 1024 * 1024
        ),
    )(*operands)
    return pl.pallas_call(
        place,
        out_shape=(
            jax.ShapeDtypeStruct((rows, key_width), BF16),
            jax.ShapeDtypeStruct((rows, width), BF16),
            jax.ShapeDtypeStruct((chunk, key_width), F32),
        ),
        in_specs=[smem] + [vmem] * 3,
        out_specs=(hbm,) * 3,
        scratch_shapes=[dma((n + 2,))],
        compiler_params=pltpu.CompilerParams(vmem_limit_bytes=8 * 1024 * 1024),
    )(order, key, ig, gb)


def body(normed, kv_cotangent, kv_weight, main_grad, owner_order):
    micro_count, tok_dev, width = normed.shape
    shard_rows, key_width = kv_weight.shape
    n = lax.axis_size("fsdp")
    dp = lax.axis_size("dp")
    rows = micro_count * tok_dev
    half = key_width // 2
    depth = n // 4
    scale = 1.0 / math.sqrt(rows * n * dp)
    chunk = shard_rows if shard_rows % 128 == 0 else max(shard_rows, 256)
    if depth == 4 and shard_rows % 128 == 0:
        key, ig, gb = near(
            normed.reshape(rows, width), kv_cotangent.reshape(rows, key_width), kv_weight, main_grad, owner_order, n, dp, scale
        )
        return (
            key.reshape(micro_count, tok_dev, key_width),
            ig.reshape(micro_count, tok_dev, width),
            gb,
        )
    x = reorder(normed.reshape(rows, width), owner_order, False)
    chunks = width // chunk
    dma = pltpu.SemaphoreType.DMA
    half_block = (shard_rows, half)
    any_spec = pl.BlockSpec(memory_space=pl.ANY)
    key, ig, gb = pl.pallas_call(
        functools.partial(kernel, n, dp, chunk, scale),
        out_shape=(
            jax.ShapeDtypeStruct((rows, key_width), BF16),
            jax.ShapeDtypeStruct((rows, width), BF16),
            jax.ShapeDtypeStruct((shard_rows, key_width), F32),
        ),
        in_specs=[any_spec] * 4,
        out_specs=(any_spec,) * 3,
        scratch_shapes=[
            pltpu.VMEM((2, rows, width), BF16),
            pltpu.VMEM((2, rows, key_width), BF16),
            pltpu.VMEM((2 * rows, half), BF16),
            pltpu.VMEM((2, n) + half_block, BF16),
            pltpu.VMEM((n,) + half_block, BF16),
            pltpu.VMEM((2, depth) + half_block, BF16),
            pltpu.VMEM((depth,) + half_block, BF16),
            pltpu.VMEM((depth,) + half_block, BF16),
            pltpu.VMEM((depth,) + half_block, BF16),
            pltpu.VMEM((depth,) + half_block, BF16),
            pltpu.VMEM((dp,) + half_block, F32),
            pltpu.VMEM((shard_rows, key_width), F32),
            pltpu.VMEM((shard_rows, key_width), F32),
            pltpu.VMEM((rows, key_width), BF16),
            pltpu.VMEM((rows, width), BF16),
            pltpu.VMEM((rows, key_width), F32),
            dma((5,)),
            dma((chunks + 2,)),
            dma,
            dma((2,)),
            dma((depth,)),
            dma((depth,)),
            dma((2 * depth,)),
            dma((n,)),
            dma((2, depth)),
            dma((depth,)),
            dma((depth,)),
            dma((dp,)),
        ],
        compiler_params=pltpu.CompilerParams(
            collective_id=0, has_side_effects=True
        ),
    )(x, kv_cotangent.reshape(rows, key_width), kv_weight, main_grad)
    ig = reorder(ig, owner_order, True)
    return (
        key.reshape(micro_count, tok_dev, key_width),
        ig.reshape(micro_count, tok_dev, width),
        gb,
    )


def solution(mesh):
    in_specs = (
        P(None, ("fsdp", "dp"), None),
        P(None, ("fsdp", "dp"), None),
        P("fsdp", None),
        P("fsdp", None),
        P(),
    )
    out_specs = (P(None, ("fsdp", "dp"), None), P(None, ("fsdp", "dp"), None), P("fsdp", None))
    return jax.shard_map(body, mesh=mesh, in_specs=in_specs, out_specs=out_specs, check_vma=False)
```

```python
import functools
import math

import jax
import jax.numpy as jnp
from jax import lax
from jax.experimental import pallas as pl
from jax.experimental.pallas import tpu as pltpu
from jax.sharding import PartitionSpec as P

MESH = pl.DeviceIdType.MESH
F32 = jnp.float32
BF16 = jnp.bfloat16
SLOT = (0, 1, 1, 2)
SWAP = (0, 2, 1, 3)


def kernel(
    n, dp, chunk, scale,
    x_hbm, c_hbm, w_hbm, main_hbm,
    key_hbm, ig_hbm, gb_hbm,
    xx, cc, ck, gath, part, r1, t1, r2, t2, r3, fin, main, gb, key, ig, acc,
    load_sem, out_sem, send_sem, x_recv, az_recv, a1_recv, a2_recv, ad_recv, r1_recv, r2_recv, r3_recv, rd_recv,
):
    f = lax.axis_index("fsdp")
    d = lax.axis_index("dp")
    k = lax.rem(d, 2)
    sib = d + 1 - 2 * k
    rows, width = x_hbm.shape
    key_width = c_hbm.shape[1]
    half = key_width // 2
    depth = n // 4
    chunks = width // chunk
    z = lax.div(f, 4)
    low = lax.rem(f, 4)
    bit0 = lax.rem(low, 2)
    bit1 = lax.div(low, 2)
    flip_x = low + 1 - 2 * bit0
    flip_y = low + 2 - 4 * bit1
    low1 = flip_x + k * (flip_y - flip_x)
    low2 = flip_y + k * (flip_x - flip_y)
    low12 = 3 - low
    p1 = z * 4 + low1
    p2 = z * 4 + low2
    steps = sorted(range(1, depth), key=lambda s: (min(s, depth - s), s))

    def peer(s):
        return lax.rem(z + s, depth)

    def dev(fi, di):
        return {"fsdp": fi, "dp": di}

    loads = []

    def load(src, dst, i):
        cp = pltpu.make_async_copy(src, dst, load_sem.at[i])
        cp.start()
        loads.append(cp)

    load(w_hbm.at[:, pl.ds(0, half)], gath.at[0, f], 0)
    load(w_hbm.at[:, pl.ds(half, half)], gath.at[1, f], 1)
    load(c_hbm, cc.at[0], 2)
    load(x_hbm, xx.at[0], 3)
    load(main_hbm, main, 4)

    barrier = pltpu.get_barrier_semaphore()
    greeted = [dev(peer(s) * 4 + low, d) for s in steps]
    greeted += [dev(p1, d), dev(p2, d)]
    greeted += [dev(f, lax.rem(d + s, dp)) for s in range(1, dp)]
    for g in greeted:
        pl.semaphore_signal(barrier, inc=1, device_id=g, device_id_type=MESH)
    pl.semaphore_wait(barrier, len(greeted))

    sent = []

    def send(src, dst, rsem, to):
        cp = pltpu.make_async_remote_copy(
            src_ref=src, dst_ref=dst, send_sem=send_sem, recv_sem=rsem, device_id=to, device_id_type=MESH
        )
        cp.start()
        sent.append(cp)

    def arrived(dst, rsem, frm):
        pltpu.make_async_remote_copy(
            src_ref=dst, dst_ref=dst, send_sem=send_sem, recv_sem=rsem, device_id=frm, device_id_type=MESH
        ).wait_recv()

    to_sib = dev(f, sib)
    to1 = dev(p1, d)
    to2 = dev(p2, d)

    send(x_hbm, xx.at[1], x_recv.at[0], to_sib)
    send(c_hbm, cc.at[1], x_recv.at[1], to_sib)
    loads[0].wait()
    loads[1].wait()

    def block(fi):
        return gath.at[k, fi]

    send(block(f), block(f), a1_recv.at[z], to1)
    send(block(f), block(f), a2_recv.at[z], to2)
    for s in steps:
        send(block(f), block(f), az_recv.at[z], dev(peer(s) * 4 + low, d))

    loads[2].wait()
    loads[3].wait()
    arrived(cc.at[1], x_recv.at[1], to_sib)
    arrived(xx.at[1], x_recv.at[0], to_sib)
    side = pl.ds(pl.multiple_of(k * half, half), half)
    ck[...] = cc[:, :, side].reshape(2 * rows, half)

    per = chunk // part.shape[1]
    ring = steps + [0]
    blockwise = per == 1

    def partial(cols):
        both = xx[:, :, cols].reshape(2 * rows, chunk)
        prod = lax.dot_general(both, ck[...], (((0,), (0,)), ((), ())), preferred_element_type=F32)
        return prod.astype(BF16)

    def feature_block(fb):
        return pl.ds(pl.multiple_of(fb * chunk, chunk), chunk)

    def partials(lo):
        if blockwise:
            for s in ring:
                fb = peer(s) * 4 + lo
                part[fb] = partial(feature_block(fb))
                if lo is low12:
                    send(part.at[fb], r1.at[0, peer(s)], r1_recv.at[0, peer(s)], to1)
                if lo is low1:
                    send(part.at[fb], r1.at[1, peer(s)], r1_recv.at[1, peer(s)], to1)

    if not blockwise:
        for j in range(chunks):
            made = partial(pl.ds(j * chunk, chunk))
            part[j * per : (j + 1) * per] = made.reshape(per, part.shape[1], half)
        for s in ring:
            send(part.at[peer(s) * 4 + low12], r1.at[0, peer(s)], r1_recv.at[0, peer(s)], to1)
    partials(low12)
    for s in steps:
        zb = peer(s)
        fb = zb * 4 + low
        arrived(block(fb), az_recv.at[zb], dev(fb, d))
        send(block(fb), block(fb), a1_recv.at[zb], to1)
        send(block(fb), block(fb), a2_recv.at[zb], to2)
        send(block(fb), block(fb), ad_recv.at[fb], to_sib)
    if not blockwise:
        for s in ring:
            send(part.at[peer(s) * 4 + low1], r1.at[1, peer(s)], r1_recv.at[1, peer(s)], to1)
    partials(low1)
    partials(low2)
    partials(low)

    outs = []

    def put(src, dst, i):
        cp = pltpu.make_async_copy(src, dst, out_sem.at[i])
        cp.start()
        outs.append(cp)

    contract = (((1,), (1,)), ((), ()))

    def from_sib(lo):
        for s in [0] + steps:
            fb = peer(s) * 4 + lo
            if s or lo is not low:
                arrived(gath.at[1 - k, fb], ad_recv.at[fb], to_sib)

    def use(lo):
        if not blockwise:
            return
        from_sib(lo)
        for s in [0] + steps:
            fb = peer(s) * 4 + lo
            cols = feature_block(fb)
            w0 = gath[0, fb]
            w1 = gath[1, fb]
            prod = lax.dot_general(cc[0, :, :half], w0, contract, preferred_element_type=F32)
            prod = prod + lax.dot_general(cc[0, :, half:], w1, contract, preferred_element_type=F32)
            ig[:, cols] = prod.astype(BF16)
            put(ig.at[:, cols], ig_hbm.at[:, cols], len(outs))
            xb = xx[0, :, cols]
            k0 = jnp.dot(xb, w0, preferred_element_type=F32)
            k1 = jnp.dot(xb, w1, preferred_element_type=F32)
            if s == 0 and lo is low:
                acc[:, :half] = k0
                acc[:, half:] = k1
            else:
                acc[:, :half] += k0
                acc[:, half:] += k1

    for s in [0] + steps:
        zb = peer(s)
        fb = zb * 4 + low1
        arrived(block(fb), a1_recv.at[zb], to1)
        send(block(fb), block(fb), a2_recv.at[depth + zb], to2)
        send(block(fb), block(fb), ad_recv.at[fb], to_sib)
    for s in ring:
        zb = peer(s)
        arrived(r1.at[0, zb], r1_recv.at[0, zb], to1)
        t1[zb] = (part[zb * 4 + low2].astype(F32) + r1[0, zb].astype(F32)).astype(BF16)
        send(t1.at[zb], r2.at[zb], r2_recv.at[zb], to2)
    use(low)
    for s in steps:
        zb = peer(s)
        arrived(r1.at[1, zb], r1_recv.at[1, zb], to1)
        arrived(r2.at[zb], r2_recv.at[zb], to2)
        t2[zb] = (part[zb * 4 + low].astype(F32) + r1[1, zb].astype(F32) + r2[zb].astype(F32)).astype(BF16)
        send(t2.at[zb], r3.at[z], r3_recv.at[z], dev(zb * 4 + low, d))
    for s in [0] + steps:
        zb = peer(s)
        fb = zb * 4 + low2
        arrived(block(fb), a2_recv.at[zb], to2)
        send(block(fb), block(fb), ad_recv.at[fb], to_sib)
    use(low1)
    use(low2)
    for s in [0] + steps:
        zb = peer(s)
        fb = zb * 4 + low12
        arrived(block(fb), a2_recv.at[depth + zb], to2)
        send(block(fb), block(fb), ad_recv.at[fb], to_sib)

    arrived(r1.at[1, z], r1_recv.at[1, z], to1)
    arrived(r2.at[z], r2_recv.at[z], to2)
    total = part[f].astype(F32) + r1[1, z].astype(F32) + r2[z].astype(F32)
    for s in steps:
        arrived(r3.at[peer(s)], r3_recv.at[peer(s)], dev(peer(s) * 4 + low, d))
        total = total + r3[peer(s)].astype(F32)
    fin[d] = total
    for s in range(1, dp):
        send(fin.at[d], fin.at[d], rd_recv.at[d], dev(f, lax.rem(d + s, dp)))

    use(low12)
    if blockwise:
        key[...] = acc[...].astype(BF16)
    else:
        for lo in (low, low1, low2, low12):
            from_sib(lo)
        for j in range(chunks):
            w0 = gath[0, j * per : (j + 1) * per].reshape(chunk, half)
            w1 = gath[1, j * per : (j + 1) * per].reshape(chunk, half)
            prod = lax.dot_general(cc[0, :, :half], w0, contract, preferred_element_type=F32)
            prod = prod + lax.dot_general(cc[0, :, half:], w1, contract, preferred_element_type=F32)
            ig[:, j * chunk : (j + 1) * chunk] = prod.astype(BF16)
        put(ig, ig_hbm, 0)
        for h in range(2):
            w = gath[h].reshape(width, half)
            key[:, h * half : (h + 1) * half] = jnp.dot(xx[0], w, preferred_element_type=F32).astype(BF16)
    put(key, key_hbm, len(outs))

    for s in range(1, dp):
        src = lax.rem(d + s, dp)
        arrived(fin.at[src], rd_recv.at[src], dev(f, src))
    loads[4].wait()
    for h in range(2):
        total = fin[h]
        for g in range(1, dp // 2):
            total = total + fin[2 * g + h]
        cols = slice(h * half, (h + 1) * half)
        gb[:, cols] = main[:, cols] + total * scale
    put(gb, gb_hbm, len(outs))
    for cp in sent:
        cp.wait_send()
    for cp in outs:
        cp.wait()


def reorder_kernel(depth, scatter, order_ref, x_ref, y_ref):
    for j in range(x_ref.shape[1] // depth):
        here = slice(j * depth, (j + 1) * depth)
        there = pl.ds(pl.multiple_of(order_ref[j] * depth, depth), depth)
        if scatter:
            y_ref[:, there] = x_ref[:, here]
        else:
            y_ref[:, here] = x_ref[:, there]


def reorder(x, order, scatter):
    rows, width = x.shape
    n = order.shape[0]
    depth = width // n
    if depth % 128:
        if scatter:
            order = jnp.argsort(order)
        return jnp.take(x.reshape(rows, n, depth), order, axis=1, mode="clip").reshape(rows, width)
    tile = rows // 4
    spec = pl.BlockSpec((tile, width), lambda i: (i, 0))
    return pl.pallas_call(
        functools.partial(reorder_kernel, depth, scatter),
        grid=(rows // tile,),
        out_shape=jax.ShapeDtypeStruct((rows, width), x.dtype),
        in_specs=[pl.BlockSpec(memory_space=pltpu.SMEM), spec],
        out_specs=spec,
        cost_estimate=pl.CostEstimate(flops=0, bytes_accessed=4 * rows * width, transcendentals=0),
    )(order, x)


def exchange(
    n, dp, scale,
    order_hbm, x_hbm, c_hbm, w_hbm, main_hbm,
    key, ig, gb, order,
    xx, cc, ck, gath, mine, give, take, part, r1, hop, zin, t3, r3, fin, main, acc,
    load_sem, send_sem, ag_recv, b_recv, sib_recv, take_recv, r1_recv, z_recv, r3_recv, fin_recv,
):
    f = lax.axis_index("fsdp")
    d = lax.axis_index("dp")
    k = lax.rem(d, 2)
    sib = d + 1 - 2 * k
    chunk, key_width = main_hbm.shape
    half = key_width // 2
    part_rows = chunk // 2
    depth = n // 4
    z = lax.div(f, 4)
    low = lax.rem(f, 4)
    bit0 = lax.rem(low, 2)
    bit1 = lax.div(low, 2)
    flip0 = low + 1 - 2 * bit0
    flip1 = low + 2 - 4 * bit1
    low_a = flip0 + k * (flip1 - flip0)
    low_b = flip1 + k * (flip0 - flip1)
    low_ab = 3 - low
    lows = (low, low_a, low_b, low_ab)
    upper = lax.div(2 * z, depth)
    has_up = z < depth - 1
    has_dn = z > 0
    mid = jnp.logical_and(has_up, has_dn)

    def close(i):
        up = i + jnp.where(i >= z, 1, 0)
        dn = depth - 1 - i - jnp.where(depth - 1 - i <= z, 1, 0)
        return (1 - upper) * up + upper * dn

    def far(t):
        return close(depth - 2 - t) if t < depth - 1 else z

    def dev(fi, di):
        return {"fsdp": fi, "dp": di}

    to_a = dev(z * 4 + low_a, d)
    to_b = dev(z * 4 + low_b, d)
    to_sib = dev(f, sib)

    def level(zi):
        return dev(lax.rem(zi + depth, depth) * 4 + low, d)

    def load(src, dst, i):
        pltpu.make_async_copy(src, dst, load_sem.at[i]).start()

    load(w_hbm.at[:, pl.ds(0, half)], gath.at[0, z, 0], 0)
    load(w_hbm.at[:, pl.ds(half, half)], gath.at[1, z, 0], 0)
    load(order_hbm, order, 1)
    load(c_hbm, cc, 2)
    for j in range(n):
        load(x_hbm.at[:, pl.ds(j * chunk, chunk)], xx.at[j], 3)
    load(main_hbm, main, 4)

    barrier = pltpu.get_barrier_semaphore()

    def greet(to):
        pl.semaphore_signal(barrier, inc=1, device_id=to, device_id_type=MESH)

    greet(to_a)
    greet(to_b)
    for s in range(1, dp):
        greet(dev(f, lax.rem(d + s, dp)))

    @pl.when(has_up)
    def _():
        greet(level(z + 1))

    @pl.when(has_dn)
    def _():
        greet(level(z - 1))

    pl.semaphore_wait(barrier, dp + 1 + jnp.where(has_up, 1, 0) + jnp.where(has_dn, 1, 0))

    sent = []

    def send(src, dst, rsem, to, cond=None):
        cp = pltpu.make_async_remote_copy(
            src_ref=src, dst_ref=dst, send_sem=send_sem, recv_sem=rsem, device_id=to, device_id_type=MESH
        )
        if cond is None:
            cp.start()
        else:
            pl.when(cond)(cp.start)
        return cp, cond

    def post(*args):
        sent.append(send(*args))

    def arrived(dst, rsem):
        pltpu.make_async_remote_copy(
            src_ref=dst, dst_ref=dst, send_sem=send_sem, recv_sem=rsem, device_id=to_sib, device_id_type=MESH
        ).wait_recv()

    def rows_of(p):
        return pl.ds(p * part_rows, part_rows)

    def forward(zz, kind):
        send(gath.at[k, zz, kind], gath.at[k, zz, kind + 2], b_recv.at[kind, zz], to_b)

    def forward_piece(zz, kind, there, p, to, cond=None):
        src = gath.at[k, zz, kind, rows_of(p)]
        dst = gath.at[k, zz, there, rows_of(p)]
        send(src, dst, ag_recv.at[there, zz, p], to, cond)

    def forward_sib(zz, kind):
        send(gath.at[k, zz, kind], gath.at[k, zz, SWAP[kind]], sib_recv.at[SLOT[kind], zz], to_sib)

    contract_rows = (((0,), (0,)), ((), ()))
    contract_cols = (((1,), (1,)), ((), ()))

    def partial(kind, t):
        zz = far(t)
        prod = lax.dot_general(xx[order[zz * 4 + lows[kind]]], ck[...], contract_rows, preferred_element_type=F32)
        give[zz, kind] = prod[:, half:].astype(BF16)
        there = 3 - SWAP[kind]
        send(give.at[zz, kind], take.at[zz, there], take_recv.at[there // 2, zz], to_sib)
        mine[zz, kind] = prod[:, :half]

    def taken(group, zz):
        arrived(take.at[zz, pl.ds(2 * group, 2)], take_recv.at[group, zz])

    def pair(zz, kind, span):
        return mine[zz, kind, span] + take[zz, 3 - kind, span].astype(F32)

    def across(j, t):
        zz = far(t)
        if j:
            taken(0, zz)
        part[j, zz] = pair(zz, 2 + j, slice(None)).astype(BF16)
        send(part.at[j, zz], r1.at[j, zz], r1_recv.at[j, zz], to_b)

    def from_a(p):
        arrived(gath.at[k, z, 1, rows_of(p)], ag_recv.at[1, z, p])
        forward_piece(z, 1, 1, p, level(z + 1), has_up)
        forward_piece(z, 1, 1, p, level(z - 1), has_dn)
        if p:
            forward(z, 1)
            forward_sib(z, 1)

    def from_z(i, j, p):
        zz = close(i)
        arrived(gath.at[k, zz, j, rows_of(p)], ag_recv.at[j, zz, p])
        below = zz < z
        on = jnp.logical_or(jnp.logical_and(below, has_up), jnp.logical_and(zz > z, has_dn))
        forward_piece(zz, j, j, p, level(z + jnp.where(below, 1, -1)), on)
        if p:
            forward(zz, j)
            forward_sib(zz, j)

    def from_b(zz, j):
        arrived(gath.at[k, zz, 2 + j], b_recv.at[j, zz])
        forward_sib(zz, 2 + j)

    def ready(j, zz):
        if j:
            taken(1, zz)
        arrived(r1.at[j, zz], r1_recv.at[j, zz])

    def summed(j, zz, span):
        return pair(zz, j, span) + r1[j, zz, span].astype(F32)

    def along(t, j, p):
        zz = far(t)
        side = jnp.where(zz > z, 0, 1)
        edge = jnp.where(zz > z, z == 0, z == depth - 1)
        span = rows_of(p)
        spot = zin.at[side, zz, j, span]
        if not p:
            ready(j, zz)

        @pl.when(jnp.logical_not(edge))
        def _():
            arrived(spot, z_recv.at[zz, j, p])

        total = summed(j, zz, span) + spot[...].astype(F32)
        hop[j, zz, span] = total.astype(BF16)
        there = z + 1 - 2 * side
        slot = jnp.where(side * depth + zz == depth + there, depth, zz)
        send(hop.at[j, zz, span], spot, z_recv.at[slot, j, p], level(there))

    def settle(j, p):
        span = rows_of(p)
        if not p:
            ready(j, z)

        @pl.when(has_dn)
        def _():
            arrived(zin.at[0, z, j, span], z_recv.at[z, j, p])

        @pl.when(has_up)
        def _():
            arrived(zin.at[1, z, j, span], z_recv.at[depth, j, p])

        return summed(j, z, span) + zin[0, z, j, span].astype(F32) + zin[1, z, j, span].astype(F32)

    def use(zz, kind, first=False):
        fb = zz * 4 + lows[kind]
        w0 = gath[0, zz, kind]
        w1 = gath[1, zz, kind]
        prod = lax.dot_general(cc[:, :half], w0, contract_cols, preferred_element_type=F32)
        prod = prod + lax.dot_general(cc[:, half:], w1, contract_cols, preferred_element_type=F32)
        ig[fb] = prod.astype(BF16)
        xb = xx[order[fb]]
        k0 = jnp.dot(xb, w0, preferred_element_type=F32)
        k1 = jnp.dot(xb, w1, preferred_element_type=F32)
        if first:
            acc[:, :half] = k0
            acc[:, half:] = k1
        else:
            acc[:, :half] += k0
            acc[:, half:] += k1

    def use_when(zz, *kinds):
        arrived(gath.at[1 - k, zz, pl.ds(kinds[0], len(kinds))], sib_recv.at[SLOT[kinds[0]], zz])
        for kind in kinds:
            use(zz, kind)

    arrived(gath.at[:, z, 0], load_sem.at[0])
    for p in range(2):
        forward_piece(z, 0, 1, p, to_a)
        forward_piece(z, 0, 0, p, level(z + 1), has_up)
        forward_piece(z, 0, 0, p, level(z - 1), has_dn)

    @pl.when(z == 0)
    def _():
        zin[0] = jnp.zeros(zin.shape[1:], BF16)

    @pl.when(z == depth - 1)
    def _():
        zin[1] = jnp.zeros(zin.shape[1:], BF16)

    pltpu.make_async_copy(order_hbm, order, load_sem.at[1]).wait()
    pltpu.make_async_copy(c_hbm, cc, load_sem.at[2]).wait()
    arrived(xx, load_sem.at[3])
    ck[:, :half] = cc[:, pl.ds(pl.multiple_of(k * half, half), half)]
    ck[:, half:] = cc[:, pl.ds(pl.multiple_of((1 - k) * half, half), half)]
    def start(*tasks):
        for what, t in tasks:
            if what == "p":
                partial(3, t)
                partial(1, t)
                partial(2, t)
            else:
                across(1, t)
                across(0, t)

    start(("p", 0))
    partial(3, 1)
    forward(z, 0)
    partial(1, 1)
    partial(2, 1)
    start(("s", 0), ("p", 2))
    from_a(0)
    start(("s", 1))
    from_a(1)
    start(("p", 3), ("s", 2))
    for p in range(2):
        from_z(0, 0, p)

        @pl.when(mid)
        def _():
            from_z(1, 0, p)

    start(("s", 3))
    partial(0, 0)
    partial(0, 1)

    def both(fn, *args):
        fn(*args, 0)
        fn(*args, 1)

    @pl.when(jnp.logical_not(mid))
    def _():
        both(along, 0, 1)
        partial(0, 2)
        both(along, 0, 0)
        both(from_z, 0, 1)
        both(along, 1, 1)
        partial(0, 3)
        use(z, 0, True)
        both(along, 1, 0)
        both(from_z, 1, 0)
        from_b(z, 0)
        use_when(close(0), 0)
        from_z(1, 1, 0)
        both(along, 2, 1)
        from_z(1, 1, 1)
        both(along, 2, 0)
        use_when(close(1), 0)
        both(from_z, 2, 0)
        from_b(z, 1)
        use_when(z, 1, 2)
        from_b(close(0), 0)
        both(from_z, 2, 1)

    @pl.when(mid)
    def _():
        partial(0, 2)
        from_z(0, 1, 0)
        from_z(1, 1, 0)
        from_z(0, 1, 1)
        from_z(1, 1, 1)
        partial(0, 3)
        use(z, 0, True)
        both(from_z, 2, 0)
        both(along, 0, 1)
        from_b(z, 0)
        use_when(close(0), 0)
        along(0, 0, 0)
        from_z(2, 1, 0)
        along(0, 0, 1)
        from_z(2, 1, 1)
        use_when(close(1), 0)
        both(along, 2, 1)
        both(along, 1, 1)
        from_b(z, 1)
        both(along, 2, 0)
        use_when(z, 1, 2)
        from_b(close(0), 0)
        both(along, 1, 0)

    use_when(close(2), 0)
    use_when(z, 3)
    for p in range(2):
        t3[rows_of(p)] = settle(1, p).astype(BF16)
        send(t3.at[rows_of(p)], r3.at[rows_of(p)], r3_recv.at[p], to_a)
    from_b(close(0), 1)
    use_when(close(0), 1, 2)
    from_b(close(1), 0)
    use_when(close(0), 3)
    from_b(close(1), 1)
    use_when(close(1), 1, 2)
    from_b(close(2), 0)
    use_when(close(1), 3)
    for p in range(2):
        fin[d, rows_of(p)] = settle(0, p)
    for p in range(2):
        arrived(r3.at[rows_of(p)], r3_recv.at[p])
        fin[d, rows_of(p)] += r3[rows_of(p)].astype(F32)
    for s in range(1, dp):
        send(fin.at[d], fin.at[d], fin_recv.at[d], dev(f, lax.rem(d + s, dp)))
    from_b(close(2), 1)
    use_when(close(2), 1, 2)
    pltpu.make_async_copy(main_hbm, main, load_sem.at[4]).wait()
    for s in range(1, dp):
        src = lax.rem(d + s, dp)
        arrived(fin.at[src], fin_recv.at[src])
    for h in range(2):
        total = fin[h]
        for g in range(1, dp // 2):
            total = total + fin[2 * g + h]
        side = slice(h * half, (h + 1) * half)
        gb[:, side] = main[:, side] + total * scale
    use_when(close(2), 3)
    key[...] = acc[...].astype(BF16)

    def send_done(src):
        pltpu.make_async_remote_copy(
            src_ref=src, dst_ref=src, send_sem=send_sem, recv_sem=r3_recv.at[0], device_id=to_sib, device_id_type=MESH
        ).wait_send()

    def left(_, carry):
        send_done(give.at[0, 0])
        return carry

    blocks = 4 + 6 * (depth - 1) + 8 * depth + 1
    for _ in range(blocks // n):
        send_done(give)
    per_z = jnp.where(has_up, z + 1, 0) + jnp.where(has_dn, depth - z, 0)
    lax.fori_loop(0, blocks % n + 2 * per_z, left, 0)
    for s in range(1, dp):
        send_done(fin.at[d])


def place(order, key, ig, gb, key_hbm, ig_hbm, gb_hbm, sem):
    n, _, chunk = ig.shape
    for fb in range(n):
        there = pl.ds(pl.multiple_of(order[fb] * chunk, chunk), chunk)
        pltpu.make_async_copy(ig.at[fb], ig_hbm.at[:, there], sem.at[0]).start()
    rest = [pltpu.make_async_copy(gb, gb_hbm, sem.at[1]), pltpu.make_async_copy(key, key_hbm, sem.at[2])]
    for cp in rest:
        cp.start()
    pltpu.make_async_copy(ig_hbm, ig_hbm, sem.at[0]).wait()
    for cp in rest:
        cp.wait()


def near(x, c, w, main, order, n, dp, scale):
    rows, width = x.shape
    chunk, key_width = main.shape
    half = key_width // 2
    depth = n // 4
    dma = pltpu.SemaphoreType.DMA
    block = (chunk, half)
    hbm = pl.BlockSpec(memory_space=pltpu.HBM)
    smem = pl.BlockSpec(memory_space=pltpu.SMEM)
    vmem = pl.BlockSpec(memory_space=pltpu.VMEM)
    operands = [pltpu.with_memory_space_constraint(a, pltpu.HBM) for a in (order, x, c, w, main)]
    key, ig, gb, order = pl.pallas_call(
        functools.partial(exchange, n, dp, scale),
        out_shape=(
            pltpu.VMEM((rows, key_width), BF16),
            pltpu.VMEM((n, rows, chunk), BF16),
            pltpu.VMEM((chunk, key_width), F32),
            pltpu.SMEM((n,), jnp.int32),
        ),
        in_specs=[hbm] * 5,
        out_specs=(vmem,) * 3 + (smem,),
        scratch_shapes=[
            pltpu.VMEM((n, rows, chunk), BF16),
            pltpu.VMEM((rows, key_width), BF16),
            pltpu.VMEM((rows, key_width), BF16),
            pltpu.VMEM((2, depth, 4) + block, BF16),
            pltpu.VMEM((depth, 4) + block, F32),
            pltpu.VMEM((depth, 4) + block, BF16),
            pltpu.VMEM((depth, 4) + block, BF16),
            pltpu.VMEM((2, depth) + block, BF16),
            pltpu.VMEM((2, depth) + block, BF16),
            pltpu.VMEM((2, depth) + block, BF16),
            pltpu.VMEM((2, depth, 2) + block, BF16),
            pltpu.VMEM(block, BF16),
            pltpu.VMEM(block, BF16),
            pltpu.VMEM((dp,) + block, F32),
            pltpu.VMEM((chunk, key_width), F32),
            pltpu.VMEM((rows, key_width), F32),
            dma((5,)),
            dma,
            dma((2, depth, 2)),
            dma((2, depth)),
            dma((3, depth)),
            dma((2, depth)),
            dma((2, depth)),
            dma((depth + 1, 2, 2)),
            dma((2,)),
            dma((dp,)),
        ],
        compiler_params=pltpu.CompilerParams(
            collective_id=0, has_side_effects=True, vmem_limit_bytes=36 * 1024 * 1024
        ),
    )(*operands)
    return pl.pallas_call(
        place,
        out_shape=(
            jax.ShapeDtypeStruct((rows, key_width), BF16),
            jax.ShapeDtypeStruct((rows, width), BF16),
            jax.ShapeDtypeStruct((chunk, key_width), F32),
        ),
        in_specs=[smem] + [vmem] * 3,
        out_specs=(hbm,) * 3,
        scratch_shapes=[dma((3,))],
        compiler_params=pltpu.CompilerParams(vmem_limit_bytes=8 * 1024 * 1024),
    )(order, key, ig, gb)


def body(normed, kv_cotangent, kv_weight, main_grad, owner_order):
    micro_count, tok_dev, width = normed.shape
    shard_rows, key_width = kv_weight.shape
    n = lax.axis_size("fsdp")
    dp = lax.axis_size("dp")
    rows = micro_count * tok_dev
    half = key_width // 2
    depth = n // 4
    scale = 1.0 / math.sqrt(rows * n * dp)
    chunk = shard_rows if shard_rows % 128 == 0 else max(shard_rows, 256)
    if depth == 4 and shard_rows % 128 == 0:
        key, ig, gb = near(
            normed.reshape(rows, width), kv_cotangent.reshape(rows, key_width), kv_weight, main_grad, owner_order, n, dp, scale
        )
        return (
            key.reshape(micro_count, tok_dev, key_width),
            ig.reshape(micro_count, tok_dev, width),
            gb,
        )
    x = reorder(normed.reshape(rows, width), owner_order, False)
    chunks = width // chunk
    dma = pltpu.SemaphoreType.DMA
    half_block = (shard_rows, half)
    any_spec = pl.BlockSpec(memory_space=pl.ANY)
    key, ig, gb = pl.pallas_call(
        functools.partial(kernel, n, dp, chunk, scale),
        out_shape=(
            jax.ShapeDtypeStruct((rows, key_width), BF16),
            jax.ShapeDtypeStruct((rows, width), BF16),
            jax.ShapeDtypeStruct((shard_rows, key_width), F32),
        ),
        in_specs=[any_spec] * 4,
        out_specs=(any_spec,) * 3,
        scratch_shapes=[
            pltpu.VMEM((2, rows, width), BF16),
            pltpu.VMEM((2, rows, key_width), BF16),
            pltpu.VMEM((2 * rows, half), BF16),
            pltpu.VMEM((2, n) + half_block, BF16),
            pltpu.VMEM((n,) + half_block, BF16),
            pltpu.VMEM((2, depth) + half_block, BF16),
            pltpu.VMEM((depth,) + half_block, BF16),
            pltpu.VMEM((depth,) + half_block, BF16),
            pltpu.VMEM((depth,) + half_block, BF16),
            pltpu.VMEM((depth,) + half_block, BF16),
            pltpu.VMEM((dp,) + half_block, F32),
            pltpu.VMEM((shard_rows, key_width), F32),
            pltpu.VMEM((shard_rows, key_width), F32),
            pltpu.VMEM((rows, key_width), BF16),
            pltpu.VMEM((rows, width), BF16),
            pltpu.VMEM((rows, key_width), F32),
            dma((5,)),
            dma((chunks + 2,)),
            dma,
            dma((2,)),
            dma((depth,)),
            dma((depth,)),
            dma((2 * depth,)),
            dma((n,)),
            dma((2, depth)),
            dma((depth,)),
            dma((depth,)),
            dma((dp,)),
        ],
        compiler_params=pltpu.CompilerParams(
            collective_id=0, has_side_effects=True
        ),
    )(x, kv_cotangent.reshape(rows, key_width), kv_weight, main_grad)
    ig = reorder(ig, owner_order, True)
    return (
        key.reshape(micro_count, tok_dev, key_width),
        ig.reshape(micro_count, tok_dev, width),
        gb,
    )


def solution(mesh):
    in_specs = (
        P(None, ("fsdp", "dp"), None),
        P(None, ("fsdp", "dp"), None),
        P("fsdp", None),
        P("fsdp", None),
        P(),
    )
    out_specs = (P(None, ("fsdp", "dp"), None), P(None, ("fsdp", "dp"), None), P("fsdp", None))
    return jax.shard_map(body, mesh=mesh, in_specs=in_specs, out_specs=out_specs, check_vma=False)
```

```python
import functools
import math

import jax
import jax.numpy as jnp
from jax import lax
from jax.experimental import pallas as pl
from jax.experimental.pallas import tpu as pltpu
from jax.sharding import PartitionSpec as P

MESH = pl.DeviceIdType.MESH
F32 = jnp.float32
BF16 = jnp.bfloat16
SLOT = (0, 1, 1, 2)
SWAP = (0, 2, 1, 3)


def kernel(
    n, dp, chunk, scale,
    x_hbm, c_hbm, w_hbm, main_hbm,
    key_hbm, ig_hbm, gb_hbm,
    xx, cc, ck, gath, part, r1, t1, r2, t2, r3, fin, main, gb, key, ig, acc,
    load_sem, out_sem, send_sem, x_recv, az_recv, a1_recv, a2_recv, ad_recv, r1_recv, r2_recv, r3_recv, rd_recv,
):
    f = lax.axis_index("fsdp")
    d = lax.axis_index("dp")
    k = lax.rem(d, 2)
    sib = d + 1 - 2 * k
    rows, width = x_hbm.shape
    key_width = c_hbm.shape[1]
    half = key_width // 2
    depth = n // 4
    chunks = width // chunk
    z = lax.div(f, 4)
    low = lax.rem(f, 4)
    bit0 = lax.rem(low, 2)
    bit1 = lax.div(low, 2)
    flip_x = low + 1 - 2 * bit0
    flip_y = low + 2 - 4 * bit1
    low1 = flip_x + k * (flip_y - flip_x)
    low2 = flip_y + k * (flip_x - flip_y)
    low12 = 3 - low
    p1 = z * 4 + low1
    p2 = z * 4 + low2
    steps = sorted(range(1, depth), key=lambda s: (min(s, depth - s), s))

    def peer(s):
        return lax.rem(z + s, depth)

    def dev(fi, di):
        return {"fsdp": fi, "dp": di}

    loads = []

    def load(src, dst, i):
        cp = pltpu.make_async_copy(src, dst, load_sem.at[i])
        cp.start()
        loads.append(cp)

    load(w_hbm.at[:, pl.ds(0, half)], gath.at[0, f], 0)
    load(w_hbm.at[:, pl.ds(half, half)], gath.at[1, f], 1)
    load(c_hbm, cc.at[0], 2)
    load(x_hbm, xx.at[0], 3)
    load(main_hbm, main, 4)

    barrier = pltpu.get_barrier_semaphore()
    greeted = [dev(peer(s) * 4 + low, d) for s in steps]
    greeted += [dev(p1, d), dev(p2, d)]
    greeted += [dev(f, lax.rem(d + s, dp)) for s in range(1, dp)]
    for g in greeted:
        pl.semaphore_signal(barrier, inc=1, device_id=g, device_id_type=MESH)
    pl.semaphore_wait(barrier, len(greeted))

    sent = []

    def send(src, dst, rsem, to):
        cp = pltpu.make_async_remote_copy(
            src_ref=src, dst_ref=dst, send_sem=send_sem, recv_sem=rsem, device_id=to, device_id_type=MESH
        )
        cp.start()
        sent.append(cp)

    def arrived(dst, rsem, frm):
        pltpu.make_async_remote_copy(
            src_ref=dst, dst_ref=dst, send_sem=send_sem, recv_sem=rsem, device_id=frm, device_id_type=MESH
        ).wait_recv()

    to_sib = dev(f, sib)
    to1 = dev(p1, d)
    to2 = dev(p2, d)

    send(x_hbm, xx.at[1], x_recv.at[0], to_sib)
    send(c_hbm, cc.at[1], x_recv.at[1], to_sib)
    loads[0].wait()
    loads[1].wait()

    def block(fi):
        return gath.at[k, fi]

    send(block(f), block(f), a1_recv.at[z], to1)
    send(block(f), block(f), a2_recv.at[z], to2)
    for s in steps:
        send(block(f), block(f), az_recv.at[z], dev(peer(s) * 4 + low, d))

    loads[2].wait()
    loads[3].wait()
    arrived(cc.at[1], x_recv.at[1], to_sib)
    arrived(xx.at[1], x_recv.at[0], to_sib)
    side = pl.ds(pl.multiple_of(k * half, half), half)
    ck[...] = cc[:, :, side].reshape(2 * rows, half)

    per = chunk // part.shape[1]
    ring = steps + [0]
    blockwise = per == 1

    def partial(cols):
        both = xx[:, :, cols].reshape(2 * rows, chunk)
        prod = lax.dot_general(both, ck[...], (((0,), (0,)), ((), ())), preferred_element_type=F32)
        return prod.astype(BF16)

    def feature_block(fb):
        return pl.ds(pl.multiple_of(fb * chunk, chunk), chunk)

    def partials(lo):
        if blockwise:
            for s in ring:
                fb = peer(s) * 4 + lo
                part[fb] = partial(feature_block(fb))
                if lo is low12:
                    send(part.at[fb], r1.at[0, peer(s)], r1_recv.at[0, peer(s)], to1)
                if lo is low1:
                    send(part.at[fb], r1.at[1, peer(s)], r1_recv.at[1, peer(s)], to1)

    if not blockwise:
        for j in range(chunks):
            made = partial(pl.ds(j * chunk, chunk))
            part[j * per : (j + 1) * per] = made.reshape(per, part.shape[1], half)
        for s in ring:
            send(part.at[peer(s) * 4 + low12], r1.at[0, peer(s)], r1_recv.at[0, peer(s)], to1)
    partials(low12)
    for s in steps:
        zb = peer(s)
        fb = zb * 4 + low
        arrived(block(fb), az_recv.at[zb], dev(fb, d))
        send(block(fb), block(fb), a1_recv.at[zb], to1)
        send(block(fb), block(fb), a2_recv.at[zb], to2)
        send(block(fb), block(fb), ad_recv.at[fb], to_sib)
    if not blockwise:
        for s in ring:
            send(part.at[peer(s) * 4 + low1], r1.at[1, peer(s)], r1_recv.at[1, peer(s)], to1)
    partials(low1)
    partials(low2)
    partials(low)

    outs = []

    def put(src, dst, i):
        cp = pltpu.make_async_copy(src, dst, out_sem.at[i])
        cp.start()
        outs.append(cp)

    contract = (((1,), (1,)), ((), ()))

    def from_sib(lo):
        for s in [0] + steps:
            fb = peer(s) * 4 + lo
            if s or lo is not low:
                arrived(gath.at[1 - k, fb], ad_recv.at[fb], to_sib)

    def use(lo):
        if not blockwise:
            return
        from_sib(lo)
        for s in [0] + steps:
            fb = peer(s) * 4 + lo
            cols = feature_block(fb)
            w0 = gath[0, fb]
            w1 = gath[1, fb]
            prod = lax.dot_general(cc[0, :, :half], w0, contract, preferred_element_type=F32)
            prod = prod + lax.dot_general(cc[0, :, half:], w1, contract, preferred_element_type=F32)
            ig[:, cols] = prod.astype(BF16)
            put(ig.at[:, cols], ig_hbm.at[:, cols], len(outs))
            xb = xx[0, :, cols]
            k0 = jnp.dot(xb, w0, preferred_element_type=F32)
            k1 = jnp.dot(xb, w1, preferred_element_type=F32)
            if s == 0 and lo is low:
                acc[:, :half] = k0
                acc[:, half:] = k1
            else:
                acc[:, :half] += k0
                acc[:, half:] += k1

    for s in [0] + steps:
        zb = peer(s)
        fb = zb * 4 + low1
        arrived(block(fb), a1_recv.at[zb], to1)
        send(block(fb), block(fb), a2_recv.at[depth + zb], to2)
        send(block(fb), block(fb), ad_recv.at[fb], to_sib)
    for s in ring:
        zb = peer(s)
        arrived(r1.at[0, zb], r1_recv.at[0, zb], to1)
        t1[zb] = (part[zb * 4 + low2].astype(F32) + r1[0, zb].astype(F32)).astype(BF16)
        send(t1.at[zb], r2.at[zb], r2_recv.at[zb], to2)
    use(low)
    for s in steps:
        zb = peer(s)
        arrived(r1.at[1, zb], r1_recv.at[1, zb], to1)
        arrived(r2.at[zb], r2_recv.at[zb], to2)
        t2[zb] = (part[zb * 4 + low].astype(F32) + r1[1, zb].astype(F32) + r2[zb].astype(F32)).astype(BF16)
        send(t2.at[zb], r3.at[z], r3_recv.at[z], dev(zb * 4 + low, d))
    for s in [0] + steps:
        zb = peer(s)
        fb = zb * 4 + low2
        arrived(block(fb), a2_recv.at[zb], to2)
        send(block(fb), block(fb), ad_recv.at[fb], to_sib)
    use(low1)
    use(low2)
    for s in [0] + steps:
        zb = peer(s)
        fb = zb * 4 + low12
        arrived(block(fb), a2_recv.at[depth + zb], to2)
        send(block(fb), block(fb), ad_recv.at[fb], to_sib)

    arrived(r1.at[1, z], r1_recv.at[1, z], to1)
    arrived(r2.at[z], r2_recv.at[z], to2)
    total = part[f].astype(F32) + r1[1, z].astype(F32) + r2[z].astype(F32)
    for s in steps:
        arrived(r3.at[peer(s)], r3_recv.at[peer(s)], dev(peer(s) * 4 + low, d))
        total = total + r3[peer(s)].astype(F32)
    fin[d] = total
    for s in range(1, dp):
        send(fin.at[d], fin.at[d], rd_recv.at[d], dev(f, lax.rem(d + s, dp)))

    use(low12)
    if blockwise:
        key[...] = acc[...].astype(BF16)
    else:
        for lo in (low, low1, low2, low12):
            from_sib(lo)
        for j in range(chunks):
            w0 = gath[0, j * per : (j + 1) * per].reshape(chunk, half)
            w1 = gath[1, j * per : (j + 1) * per].reshape(chunk, half)
            prod = lax.dot_general(cc[0, :, :half], w0, contract, preferred_element_type=F32)
            prod = prod + lax.dot_general(cc[0, :, half:], w1, contract, preferred_element_type=F32)
            ig[:, j * chunk : (j + 1) * chunk] = prod.astype(BF16)
        put(ig, ig_hbm, 0)
        for h in range(2):
            w = gath[h].reshape(width, half)
            key[:, h * half : (h + 1) * half] = jnp.dot(xx[0], w, preferred_element_type=F32).astype(BF16)
    put(key, key_hbm, len(outs))

    for s in range(1, dp):
        src = lax.rem(d + s, dp)
        arrived(fin.at[src], rd_recv.at[src], dev(f, src))
    loads[4].wait()
    for h in range(2):
        total = fin[h]
        for g in range(1, dp // 2):
            total = total + fin[2 * g + h]
        cols = slice(h * half, (h + 1) * half)
        gb[:, cols] = main[:, cols] + total * scale
    put(gb, gb_hbm, len(outs))
    for cp in sent:
        cp.wait_send()
    for cp in outs:
        cp.wait()


def reorder_kernel(depth, scatter, order_ref, x_ref, y_ref):
    for j in range(x_ref.shape[1] // depth):
        here = slice(j * depth, (j + 1) * depth)
        there = pl.ds(pl.multiple_of(order_ref[j] * depth, depth), depth)
        if scatter:
            y_ref[:, there] = x_ref[:, here]
        else:
            y_ref[:, here] = x_ref[:, there]


def reorder(x, order, scatter):
    rows, width = x.shape
    n = order.shape[0]
    depth = width // n
    if depth % 128:
        if scatter:
            order = jnp.argsort(order)
        return jnp.take(x.reshape(rows, n, depth), order, axis=1, mode="clip").reshape(rows, width)
    tile = rows // 4
    spec = pl.BlockSpec((tile, width), lambda i: (i, 0))
    return pl.pallas_call(
        functools.partial(reorder_kernel, depth, scatter),
        grid=(rows // tile,),
        out_shape=jax.ShapeDtypeStruct((rows, width), x.dtype),
        in_specs=[pl.BlockSpec(memory_space=pltpu.SMEM), spec],
        out_specs=spec,
        cost_estimate=pl.CostEstimate(flops=0, bytes_accessed=4 * rows * width, transcendentals=0),
    )(order, x)


def exchange(
    n, dp, scale,
    order_hbm, x_hbm, c_hbm, w_hbm, main_hbm,
    key, ig, gb, order,
    xx, cc, ck, gath, mine, give, take, part, r1, hop, zin, t3, r3, fin, main, acc,
    load_sem, send_sem, ag_recv, b_recv, sib_recv, take_recv, r1_recv, z_recv, r3_recv, fin_recv,
):
    f = lax.axis_index("fsdp")
    d = lax.axis_index("dp")
    k = lax.rem(d, 2)
    sib = d + 1 - 2 * k
    chunk, key_width = main_hbm.shape
    half = key_width // 2
    part_rows = chunk // 2
    depth = n // 4
    z = lax.div(f, 4)
    low = lax.rem(f, 4)
    bit0 = lax.rem(low, 2)
    bit1 = lax.div(low, 2)
    flip0 = low + 1 - 2 * bit0
    flip1 = low + 2 - 4 * bit1
    low_a = flip0 + k * (flip1 - flip0)
    low_b = flip1 + k * (flip0 - flip1)
    low_ab = 3 - low
    lows = (low, low_a, low_b, low_ab)
    upper = lax.div(2 * z, depth)
    has_up = z < depth - 1
    has_dn = z > 0
    mid = jnp.logical_and(has_up, has_dn)

    def close(i):
        up = i + jnp.where(i >= z, 1, 0)
        dn = depth - 1 - i - jnp.where(depth - 1 - i <= z, 1, 0)
        return (1 - upper) * up + upper * dn

    def far(t):
        return close(depth - 2 - t) if t < depth - 1 else z

    def dev(fi, di):
        return {"fsdp": fi, "dp": di}

    to_a = dev(z * 4 + low_a, d)
    to_b = dev(z * 4 + low_b, d)
    to_sib = dev(f, sib)

    def level(zi):
        return dev(lax.rem(zi + depth, depth) * 4 + low, d)

    def load(src, dst, i):
        pltpu.make_async_copy(src, dst, load_sem.at[i]).start()

    load(w_hbm.at[:, pl.ds(0, half)], gath.at[0, z, 0], 0)
    load(w_hbm.at[:, pl.ds(half, half)], gath.at[1, z, 0], 0)
    load(order_hbm, order, 1)
    load(c_hbm, cc, 2)
    for j in range(n):
        load(x_hbm.at[:, pl.ds(j * chunk, chunk)], xx.at[j], 3)
    load(main_hbm, main, 4)

    barrier = pltpu.get_barrier_semaphore()

    def greet(to):
        pl.semaphore_signal(barrier, inc=1, device_id=to, device_id_type=MESH)

    greet(to_a)
    greet(to_b)
    for s in range(1, dp):
        greet(dev(f, lax.rem(d + s, dp)))

    @pl.when(has_up)
    def _():
        greet(level(z + 1))

    @pl.when(has_dn)
    def _():
        greet(level(z - 1))

    pl.semaphore_wait(barrier, dp + 1 + jnp.where(has_up, 1, 0) + jnp.where(has_dn, 1, 0))

    sent = []

    def send(src, dst, rsem, to, cond=None):
        cp = pltpu.make_async_remote_copy(
            src_ref=src, dst_ref=dst, send_sem=send_sem, recv_sem=rsem, device_id=to, device_id_type=MESH
        )
        if cond is None:
            cp.start()
        else:
            pl.when(cond)(cp.start)
        return cp, cond

    def post(*args):
        sent.append(send(*args))

    def arrived(dst, rsem):
        pltpu.make_async_remote_copy(
            src_ref=dst, dst_ref=dst, send_sem=send_sem, recv_sem=rsem, device_id=to_sib, device_id_type=MESH
        ).wait_recv()

    def rows_of(p):
        return pl.ds(p * part_rows, part_rows)

    def forward(zz, kind):
        send(gath.at[k, zz, kind], gath.at[k, zz, kind + 2], b_recv.at[kind, zz], to_b)

    def forward_piece(zz, kind, there, p, to, cond=None):
        src = gath.at[k, zz, kind, rows_of(p)]
        dst = gath.at[k, zz, there, rows_of(p)]
        send(src, dst, ag_recv.at[there, zz, p], to, cond)

    def forward_sib(zz, kind):
        send(gath.at[k, zz, kind], gath.at[k, zz, SWAP[kind]], sib_recv.at[SLOT[kind], zz], to_sib)

    contract_rows = (((0,), (0,)), ((), ()))
    contract_cols = (((1,), (1,)), ((), ()))

    def partial(kind, t):
        zz = far(t)
        prod = lax.dot_general(xx[order[zz * 4 + lows[kind]]], ck[...], contract_rows, preferred_element_type=F32)
        give[zz, kind] = prod[:, half:].astype(BF16)
        there = 3 - SWAP[kind]
        send(give.at[zz, kind], take.at[zz, there], take_recv.at[there // 2, zz], to_sib)
        mine[zz, kind] = prod[:, :half]

    def taken(group, zz):
        arrived(take.at[zz, pl.ds(2 * group, 2)], take_recv.at[group, zz])

    def pair(zz, kind, span):
        return mine[zz, kind, span] + take[zz, 3 - kind, span].astype(F32)

    def across(j, t):
        zz = far(t)
        if j:
            taken(0, zz)
        part[j, zz] = pair(zz, 2 + j, slice(None)).astype(BF16)
        send(part.at[j, zz], r1.at[j, zz], r1_recv.at[j, zz], to_b)

    def from_a(p):
        arrived(gath.at[k, z, 1, rows_of(p)], ag_recv.at[1, z, p])
        forward_piece(z, 1, 1, p, level(z + 1), has_up)
        forward_piece(z, 1, 1, p, level(z - 1), has_dn)
        if p:
            forward(z, 1)
            forward_sib(z, 1)

    def from_z(i, j, p):
        zz = close(i)
        arrived(gath.at[k, zz, j, rows_of(p)], ag_recv.at[j, zz, p])
        below = zz < z
        on = jnp.logical_or(jnp.logical_and(below, has_up), jnp.logical_and(zz > z, has_dn))
        forward_piece(zz, j, j, p, level(z + jnp.where(below, 1, -1)), on)
        if p:
            forward(zz, j)
            forward_sib(zz, j)

    def from_b(zz, j):
        arrived(gath.at[k, zz, 2 + j], b_recv.at[j, zz])
        forward_sib(zz, 2 + j)

    def ready(j, zz):
        if j:
            taken(1, zz)
        arrived(r1.at[j, zz], r1_recv.at[j, zz])

    def summed(j, zz, span):
        return pair(zz, j, span) + r1[j, zz, span].astype(F32)

    def along(t, j, p):
        zz = far(t)
        side = jnp.where(zz > z, 0, 1)
        edge = jnp.where(zz > z, z == 0, z == depth - 1)
        span = rows_of(p)
        spot = zin.at[side, zz, j, span]
        if not p:
            ready(j, zz)

        @pl.when(jnp.logical_not(edge))
        def _():
            arrived(spot, z_recv.at[zz, j, p])

        total = summed(j, zz, span) + spot[...].astype(F32)
        hop[j, zz, span] = total.astype(BF16)
        there = z + 1 - 2 * side
        slot = jnp.where(side * depth + zz == depth + there, depth, zz)
        send(hop.at[j, zz, span], spot, z_recv.at[slot, j, p], level(there))

    def settle(j, p):
        span = rows_of(p)
        if not p:
            ready(j, z)

        @pl.when(has_dn)
        def _():
            arrived(zin.at[0, z, j, span], z_recv.at[z, j, p])

        @pl.when(has_up)
        def _():
            arrived(zin.at[1, z, j, span], z_recv.at[depth, j, p])

        return summed(j, z, span) + zin[0, z, j, span].astype(F32) + zin[1, z, j, span].astype(F32)

    def use(zz, kind, first=False):
        fb = zz * 4 + lows[kind]
        w0 = gath[0, zz, kind]
        w1 = gath[1, zz, kind]
        prod = lax.dot_general(cc[:, :half], w0, contract_cols, preferred_element_type=F32)
        prod = prod + lax.dot_general(cc[:, half:], w1, contract_cols, preferred_element_type=F32)
        ig[fb] = prod.astype(BF16)
        xb = xx[order[fb]]
        k0 = jnp.dot(xb, w0, preferred_element_type=F32)
        k1 = jnp.dot(xb, w1, preferred_element_type=F32)
        if first:
            acc[:, :half] = k0
            acc[:, half:] = k1
        else:
            acc[:, :half] += k0
            acc[:, half:] += k1

    def use_when(zz, *kinds):
        arrived(gath.at[1 - k, zz, pl.ds(kinds[0], len(kinds))], sib_recv.at[SLOT[kinds[0]], zz])
        for kind in kinds:
            use(zz, kind)

    arrived(gath.at[:, z, 0], load_sem.at[0])
    for p in range(2):
        forward_piece(z, 0, 1, p, to_a)
        forward_piece(z, 0, 0, p, level(z + 1), has_up)
        forward_piece(z, 0, 0, p, level(z - 1), has_dn)

    forward(z, 0)

    @pl.when(z == 0)
    def _():
        zin[0] = jnp.zeros(zin.shape[1:], BF16)

    @pl.when(z == depth - 1)
    def _():
        zin[1] = jnp.zeros(zin.shape[1:], BF16)

    pltpu.make_async_copy(order_hbm, order, load_sem.at[1]).wait()
    pltpu.make_async_copy(c_hbm, cc, load_sem.at[2]).wait()
    arrived(xx, load_sem.at[3])
    ck[:, :half] = cc[:, pl.ds(pl.multiple_of(k * half, half), half)]
    ck[:, half:] = cc[:, pl.ds(pl.multiple_of((1 - k) * half, half), half)]
    def start(*tasks):
        for what, t in tasks:
            if what == "p":
                partial(3, t)
                partial(1, t)
                partial(2, t)
            else:
                across(1, t)
                across(0, t)

    start(("p", 0))
    start(("p", 1), ("s", 0))
    partial(0, 0)
    start(("p", 2))
    from_a(0)
    start(("s", 1))
    from_a(1)
    start(("p", 3), ("s", 2))
    for p in range(2):
        from_z(0, 0, p)

        @pl.when(mid)
        def _():
            from_z(1, 0, p)

    def both(fn, *args):
        fn(*args, 0)
        fn(*args, 1)

    partial(0, 1)

    @pl.when(jnp.logical_not(mid))
    def _():
        both(along, 0, 1)

    start(("s", 3))

    @pl.when(jnp.logical_not(mid))
    def _():
        partial(0, 2)
        both(along, 0, 0)
        both(from_z, 0, 1)
        both(along, 1, 1)
        partial(0, 3)
        use(z, 0, True)
        both(along, 1, 0)
        both(from_z, 1, 0)
        from_b(z, 0)
        use_when(close(0), 0)
        from_z(1, 1, 0)
        both(along, 2, 1)
        from_z(1, 1, 1)
        both(along, 2, 0)
        use_when(close(1), 0)
        both(from_z, 2, 0)
        from_b(z, 1)
        use_when(z, 1, 2)
        from_b(close(0), 0)
        both(from_z, 2, 1)

    @pl.when(mid)
    def _():
        partial(0, 2)
        from_z(0, 1, 0)
        from_z(1, 1, 0)
        from_z(0, 1, 1)
        from_z(1, 1, 1)
        partial(0, 3)
        use(z, 0, True)
        both(from_z, 2, 0)
        both(along, 0, 1)
        from_b(z, 0)
        use_when(close(0), 0)
        along(0, 0, 0)
        from_z(2, 1, 0)
        along(0, 0, 1)
        from_z(2, 1, 1)
        use_when(close(1), 0)
        both(along, 2, 1)
        both(along, 1, 1)
        from_b(z, 1)
        both(along, 2, 0)
        use_when(z, 1, 2)
        from_b(close(0), 0)
        both(along, 1, 0)

    use_when(close(2), 0)
    use_when(z, 3)
    for p in range(2):
        t3[rows_of(p)] = settle(1, p).astype(BF16)
        send(t3.at[rows_of(p)], r3.at[rows_of(p)], r3_recv.at[p], to_a)
    from_b(close(0), 1)
    use_when(close(0), 1, 2)
    from_b(close(1), 0)
    use_when(close(0), 3)
    from_b(close(1), 1)
    use_when(close(1), 1, 2)
    from_b(close(2), 0)
    use_when(close(1), 3)
    for p in range(2):
        fin[d, rows_of(p)] = settle(0, p)
    for p in range(2):
        arrived(r3.at[rows_of(p)], r3_recv.at[p])
        fin[d, rows_of(p)] += r3[rows_of(p)].astype(F32)
    for s in range(1, dp):
        send(fin.at[d], fin.at[d], fin_recv.at[d], dev(f, lax.rem(d + s, dp)))
    from_b(close(2), 1)
    use_when(close(2), 1, 2)
    pltpu.make_async_copy(main_hbm, main, load_sem.at[4]).wait()
    for s in range(1, dp):
        src = lax.rem(d + s, dp)
        arrived(fin.at[src], fin_recv.at[src])
    for h in range(2):
        total = fin[h]
        for g in range(1, dp // 2):
            total = total + fin[2 * g + h]
        side = slice(h * half, (h + 1) * half)
        gb[:, side] = main[:, side] + total * scale
    use_when(close(2), 3)
    key[...] = acc[...].astype(BF16)

    def send_done(src):
        pltpu.make_async_remote_copy(
            src_ref=src, dst_ref=src, send_sem=send_sem, recv_sem=r3_recv.at[0], device_id=to_sib, device_id_type=MESH
        ).wait_send()

    def left(_, carry):
        send_done(give.at[0, 0])
        return carry

    blocks = 4 + 6 * (depth - 1) + 8 * depth + 1
    for _ in range(blocks // n):
        send_done(give)
    per_z = jnp.where(has_up, z + 1, 0) + jnp.where(has_dn, depth - z, 0)
    lax.fori_loop(0, blocks % n + 2 * per_z, left, 0)
    for s in range(1, dp):
        send_done(fin.at[d])


def place(order, key, ig, gb, key_hbm, ig_hbm, gb_hbm, sem):
    n, _, chunk = ig.shape
    for fb in range(n):
        there = pl.ds(pl.multiple_of(order[fb] * chunk, chunk), chunk)
        pltpu.make_async_copy(ig.at[fb], ig_hbm.at[:, there], sem.at[0]).start()
    rest = [pltpu.make_async_copy(gb, gb_hbm, sem.at[1]), pltpu.make_async_copy(key, key_hbm, sem.at[2])]
    for cp in rest:
        cp.start()
    pltpu.make_async_copy(ig_hbm, ig_hbm, sem.at[0]).wait()
    for cp in rest:
        cp.wait()


def near(x, c, w, main, order, n, dp, scale):
    rows, width = x.shape
    chunk, key_width = main.shape
    half = key_width // 2
    depth = n // 4
    dma = pltpu.SemaphoreType.DMA
    block = (chunk, half)
    hbm = pl.BlockSpec(memory_space=pltpu.HBM)
    smem = pl.BlockSpec(memory_space=pltpu.SMEM)
    vmem = pl.BlockSpec(memory_space=pltpu.VMEM)
    operands = [pltpu.with_memory_space_constraint(a, pltpu.HBM) for a in (order, x, c, w, main)]
    key, ig, gb, order = pl.pallas_call(
        functools.partial(exchange, n, dp, scale),
        out_shape=(
            pltpu.VMEM((rows, key_width), BF16),
            pltpu.VMEM((n, rows, chunk), BF16),
            pltpu.VMEM((chunk, key_width), F32),
            pltpu.SMEM((n,), jnp.int32),
        ),
        in_specs=[hbm] * 5,
        out_specs=(vmem,) * 3 + (smem,),
        scratch_shapes=[
            pltpu.VMEM((n, rows, chunk), BF16),
            pltpu.VMEM((rows, key_width), BF16),
            pltpu.VMEM((rows, key_width), BF16),
            pltpu.VMEM((2, depth, 4) + block, BF16),
            pltpu.VMEM((depth, 4) + block, F32),
            pltpu.VMEM((depth, 4) + block, BF16),
            pltpu.VMEM((depth, 4) + block, BF16),
            pltpu.VMEM((2, depth) + block, BF16),
            pltpu.VMEM((2, depth) + block, BF16),
            pltpu.VMEM((2, depth) + block, BF16),
            pltpu.VMEM((2, depth, 2) + block, BF16),
            pltpu.VMEM(block, BF16),
            pltpu.VMEM(block, BF16),
            pltpu.VMEM((dp,) + block, F32),
            pltpu.VMEM((chunk, key_width), F32),
            pltpu.VMEM((rows, key_width), F32),
            dma((5,)),
            dma,
            dma((2, depth, 2)),
            dma((2, depth)),
            dma((3, depth)),
            dma((2, depth)),
            dma((2, depth)),
            dma((depth + 1, 2, 2)),
            dma((2,)),
            dma((dp,)),
        ],
        compiler_params=pltpu.CompilerParams(
            collective_id=0, has_side_effects=True, vmem_limit_bytes=36 * 1024 * 1024
        ),
    )(*operands)
    return pl.pallas_call(
        place,
        out_shape=(
            jax.ShapeDtypeStruct((rows, key_width), BF16),
            jax.ShapeDtypeStruct((rows, width), BF16),
            jax.ShapeDtypeStruct((chunk, key_width), F32),
        ),
        in_specs=[smem] + [vmem] * 3,
        out_specs=(hbm,) * 3,
        scratch_shapes=[dma((3,))],
        compiler_params=pltpu.CompilerParams(vmem_limit_bytes=8 * 1024 * 1024),
    )(order, key, ig, gb)


def body(normed, kv_cotangent, kv_weight, main_grad, owner_order):
    micro_count, tok_dev, width = normed.shape
    shard_rows, key_width = kv_weight.shape
    n = lax.axis_size("fsdp")
    dp = lax.axis_size("dp")
    rows = micro_count * tok_dev
    half = key_width // 2
    depth = n // 4
    scale = 1.0 / math.sqrt(rows * n * dp)
    chunk = shard_rows if shard_rows % 128 == 0 else max(shard_rows, 256)
    if depth == 4 and shard_rows % 128 == 0:
        key, ig, gb = near(
            normed.reshape(rows, width), kv_cotangent.reshape(rows, key_width), kv_weight, main_grad, owner_order, n, dp, scale
        )
        return (
            key.reshape(micro_count, tok_dev, key_width),
            ig.reshape(micro_count, tok_dev, width),
            gb,
        )
    x = reorder(normed.reshape(rows, width), owner_order, False)
    chunks = width // chunk
    dma = pltpu.SemaphoreType.DMA
    half_block = (shard_rows, half)
    any_spec = pl.BlockSpec(memory_space=pl.ANY)
    key, ig, gb = pl.pallas_call(
        functools.partial(kernel, n, dp, chunk, scale),
        out_shape=(
            jax.ShapeDtypeStruct((rows, key_width), BF16),
            jax.ShapeDtypeStruct((rows, width), BF16),
            jax.ShapeDtypeStruct((shard_rows, key_width), F32),
        ),
        in_specs=[any_spec] * 4,
        out_specs=(any_spec,) * 3,
        scratch_shapes=[
            pltpu.VMEM((2, rows, width), BF16),
            pltpu.VMEM((2, rows, key_width), BF16),
            pltpu.VMEM((2 * rows, half), BF16),
            pltpu.VMEM((2, n) + half_block, BF16),
            pltpu.VMEM((n,) + half_block, BF16),
            pltpu.VMEM((2, depth) + half_block, BF16),
            pltpu.VMEM((depth,) + half_block, BF16),
            pltpu.VMEM((depth,) + half_block, BF16),
            pltpu.VMEM((depth,) + half_block, BF16),
            pltpu.VMEM((depth,) + half_block, BF16),
            pltpu.VMEM((dp,) + half_block, F32),
            pltpu.VMEM((shard_rows, key_width), F32),
            pltpu.VMEM((shard_rows, key_width), F32),
            pltpu.VMEM((rows, key_width), BF16),
            pltpu.VMEM((rows, width), BF16),
            pltpu.VMEM((rows, key_width), F32),
            dma((5,)),
            dma((chunks + 2,)),
            dma,
            dma((2,)),
            dma((depth,)),
            dma((depth,)),
            dma((2 * depth,)),
            dma((n,)),
            dma((2, depth)),
            dma((depth,)),
            dma((depth,)),
            dma((dp,)),
        ],
        compiler_params=pltpu.CompilerParams(
            collective_id=0, has_side_effects=True
        ),
    )(x, kv_cotangent.reshape(rows, key_width), kv_weight, main_grad)
    ig = reorder(ig, owner_order, True)
    return (
        key.reshape(micro_count, tok_dev, key_width),
        ig.reshape(micro_count, tok_dev, width),
        gb,
    )


def solution(mesh):
    in_specs = (
        P(None, ("fsdp", "dp"), None),
        P(None, ("fsdp", "dp"), None),
        P("fsdp", None),
        P("fsdp", None),
        P(),
    )
    out_specs = (P(None, ("fsdp", "dp"), None), P(None, ("fsdp", "dp"), None), P("fsdp", None))
    return jax.shard_map(body, mesh=mesh, in_specs=in_specs, out_specs=out_specs, check_vma=False)
```

```python
import functools
import math

import jax
import jax.numpy as jnp
from jax import lax
from jax.experimental import pallas as pl
from jax.experimental.pallas import tpu as pltpu
from jax.sharding import PartitionSpec as P

MESH = pl.DeviceIdType.MESH
F32 = jnp.float32
BF16 = jnp.bfloat16
SLOT = (0, 1, 1, 2)
SWAP = (0, 2, 1, 3)


def kernel(
    n, dp, chunk, scale,
    x_hbm, c_hbm, w_hbm, main_hbm,
    key_hbm, ig_hbm, gb_hbm,
    xx, cc, ck, gath, part, r1, t1, r2, t2, r3, fin, main, gb, key, ig, acc,
    load_sem, out_sem, send_sem, x_recv, az_recv, a1_recv, a2_recv, ad_recv, r1_recv, r2_recv, r3_recv, rd_recv,
):
    f = lax.axis_index("fsdp")
    d = lax.axis_index("dp")
    k = lax.rem(d, 2)
    sib = d + 1 - 2 * k
    rows, width = x_hbm.shape
    key_width = c_hbm.shape[1]
    half = key_width // 2
    depth = n // 4
    chunks = width // chunk
    z = lax.div(f, 4)
    low = lax.rem(f, 4)
    bit0 = lax.rem(low, 2)
    bit1 = lax.div(low, 2)
    flip_x = low + 1 - 2 * bit0
    flip_y = low + 2 - 4 * bit1
    low1 = flip_x + k * (flip_y - flip_x)
    low2 = flip_y + k * (flip_x - flip_y)
    low12 = 3 - low
    p1 = z * 4 + low1
    p2 = z * 4 + low2
    steps = sorted(range(1, depth), key=lambda s: (min(s, depth - s), s))

    def peer(s):
        return lax.rem(z + s, depth)

    def dev(fi, di):
        return {"fsdp": fi, "dp": di}

    loads = []

    def load(src, dst, i):
        cp = pltpu.make_async_copy(src, dst, load_sem.at[i])
        cp.start()
        loads.append(cp)

    load(w_hbm.at[:, pl.ds(0, half)], gath.at[0, f], 0)
    load(w_hbm.at[:, pl.ds(half, half)], gath.at[1, f], 1)
    load(c_hbm, cc.at[0], 2)
    load(x_hbm, xx.at[0], 3)
    load(main_hbm, main, 4)

    barrier = pltpu.get_barrier_semaphore()
    greeted = [dev(peer(s) * 4 + low, d) for s in steps]
    greeted += [dev(p1, d), dev(p2, d)]
    greeted += [dev(f, lax.rem(d + s, dp)) for s in range(1, dp)]
    for g in greeted:
        pl.semaphore_signal(barrier, inc=1, device_id=g, device_id_type=MESH)
    pl.semaphore_wait(barrier, len(greeted))

    sent = []

    def send(src, dst, rsem, to):
        cp = pltpu.make_async_remote_copy(
            src_ref=src, dst_ref=dst, send_sem=send_sem, recv_sem=rsem, device_id=to, device_id_type=MESH
        )
        cp.start()
        sent.append(cp)

    def arrived(dst, rsem, frm):
        pltpu.make_async_remote_copy(
            src_ref=dst, dst_ref=dst, send_sem=send_sem, recv_sem=rsem, device_id=frm, device_id_type=MESH
        ).wait_recv()

    to_sib = dev(f, sib)
    to1 = dev(p1, d)
    to2 = dev(p2, d)

    send(x_hbm, xx.at[1], x_recv.at[0], to_sib)
    send(c_hbm, cc.at[1], x_recv.at[1], to_sib)
    loads[0].wait()
    loads[1].wait()

    def block(fi):
        return gath.at[k, fi]

    send(block(f), block(f), a1_recv.at[z], to1)
    send(block(f), block(f), a2_recv.at[z], to2)
    for s in steps:
        send(block(f), block(f), az_recv.at[z], dev(peer(s) * 4 + low, d))

    loads[2].wait()
    loads[3].wait()
    arrived(cc.at[1], x_recv.at[1], to_sib)
    arrived(xx.at[1], x_recv.at[0], to_sib)
    side = pl.ds(pl.multiple_of(k * half, half), half)
    ck[...] = cc[:, :, side].reshape(2 * rows, half)

    per = chunk // part.shape[1]
    ring = steps + [0]
    blockwise = per == 1

    def partial(cols):
        both = xx[:, :, cols].reshape(2 * rows, chunk)
        prod = lax.dot_general(both, ck[...], (((0,), (0,)), ((), ())), preferred_element_type=F32)
        return prod.astype(BF16)

    def feature_block(fb):
        return pl.ds(pl.multiple_of(fb * chunk, chunk), chunk)

    def partials(lo):
        if blockwise:
            for s in ring:
                fb = peer(s) * 4 + lo
                part[fb] = partial(feature_block(fb))
                if lo is low12:
                    send(part.at[fb], r1.at[0, peer(s)], r1_recv.at[0, peer(s)], to1)
                if lo is low1:
                    send(part.at[fb], r1.at[1, peer(s)], r1_recv.at[1, peer(s)], to1)

    if not blockwise:
        for j in range(chunks):
            made = partial(pl.ds(j * chunk, chunk))
            part[j * per : (j + 1) * per] = made.reshape(per, part.shape[1], half)
        for s in ring:
            send(part.at[peer(s) * 4 + low12], r1.at[0, peer(s)], r1_recv.at[0, peer(s)], to1)
    partials(low12)
    for s in steps:
        zb = peer(s)
        fb = zb * 4 + low
        arrived(block(fb), az_recv.at[zb], dev(fb, d))
        send(block(fb), block(fb), a1_recv.at[zb], to1)
        send(block(fb), block(fb), a2_recv.at[zb], to2)
        send(block(fb), block(fb), ad_recv.at[fb], to_sib)
    if not blockwise:
        for s in ring:
            send(part.at[peer(s) * 4 + low1], r1.at[1, peer(s)], r1_recv.at[1, peer(s)], to1)
    partials(low1)
    partials(low2)
    partials(low)

    outs = []

    def put(src, dst, i):
        cp = pltpu.make_async_copy(src, dst, out_sem.at[i])
        cp.start()
        outs.append(cp)

    contract = (((1,), (1,)), ((), ()))

    def from_sib(lo):
        for s in [0] + steps:
            fb = peer(s) * 4 + lo
            if s or lo is not low:
                arrived(gath.at[1 - k, fb], ad_recv.at[fb], to_sib)

    def use(lo):
        if not blockwise:
            return
        from_sib(lo)
        for s in [0] + steps:
            fb = peer(s) * 4 + lo
            cols = feature_block(fb)
            w0 = gath[0, fb]
            w1 = gath[1, fb]
            prod = lax.dot_general(cc[0, :, :half], w0, contract, preferred_element_type=F32)
            prod = prod + lax.dot_general(cc[0, :, half:], w1, contract, preferred_element_type=F32)
            ig[:, cols] = prod.astype(BF16)
            put(ig.at[:, cols], ig_hbm.at[:, cols], len(outs))
            xb = xx[0, :, cols]
            k0 = jnp.dot(xb, w0, preferred_element_type=F32)
            k1 = jnp.dot(xb, w1, preferred_element_type=F32)
            if s == 0 and lo is low:
                acc[:, :half] = k0
                acc[:, half:] = k1
            else:
                acc[:, :half] += k0
                acc[:, half:] += k1

    for s in [0] + steps:
        zb = peer(s)
        fb = zb * 4 + low1
        arrived(block(fb), a1_recv.at[zb], to1)
        send(block(fb), block(fb), a2_recv.at[depth + zb], to2)
        send(block(fb), block(fb), ad_recv.at[fb], to_sib)
    for s in ring:
        zb = peer(s)
        arrived(r1.at[0, zb], r1_recv.at[0, zb], to1)
        t1[zb] = (part[zb * 4 + low2].astype(F32) + r1[0, zb].astype(F32)).astype(BF16)
        send(t1.at[zb], r2.at[zb], r2_recv.at[zb], to2)
    use(low)
    for s in steps:
        zb = peer(s)
        arrived(r1.at[1, zb], r1_recv.at[1, zb], to1)
        arrived(r2.at[zb], r2_recv.at[zb], to2)
        t2[zb] = (part[zb * 4 + low].astype(F32) + r1[1, zb].astype(F32) + r2[zb].astype(F32)).astype(BF16)
        send(t2.at[zb], r3.at[z], r3_recv.at[z], dev(zb * 4 + low, d))
    for s in [0] + steps:
        zb = peer(s)
        fb = zb * 4 + low2
        arrived(block(fb), a2_recv.at[zb], to2)
        send(block(fb), block(fb), ad_recv.at[fb], to_sib)
    use(low1)
    use(low2)
    for s in [0] + steps:
        zb = peer(s)
        fb = zb * 4 + low12
        arrived(block(fb), a2_recv.at[depth + zb], to2)
        send(block(fb), block(fb), ad_recv.at[fb], to_sib)

    arrived(r1.at[1, z], r1_recv.at[1, z], to1)
    arrived(r2.at[z], r2_recv.at[z], to2)
    total = part[f].astype(F32) + r1[1, z].astype(F32) + r2[z].astype(F32)
    for s in steps:
        arrived(r3.at[peer(s)], r3_recv.at[peer(s)], dev(peer(s) * 4 + low, d))
        total = total + r3[peer(s)].astype(F32)
    fin[d] = total
    for s in range(1, dp):
        send(fin.at[d], fin.at[d], rd_recv.at[d], dev(f, lax.rem(d + s, dp)))

    use(low12)
    if blockwise:
        key[...] = acc[...].astype(BF16)
    else:
        for lo in (low, low1, low2, low12):
            from_sib(lo)
        for j in range(chunks):
            w0 = gath[0, j * per : (j + 1) * per].reshape(chunk, half)
            w1 = gath[1, j * per : (j + 1) * per].reshape(chunk, half)
            prod = lax.dot_general(cc[0, :, :half], w0, contract, preferred_element_type=F32)
            prod = prod + lax.dot_general(cc[0, :, half:], w1, contract, preferred_element_type=F32)
            ig[:, j * chunk : (j + 1) * chunk] = prod.astype(BF16)
        put(ig, ig_hbm, 0)
        for h in range(2):
            w = gath[h].reshape(width, half)
            key[:, h * half : (h + 1) * half] = jnp.dot(xx[0], w, preferred_element_type=F32).astype(BF16)
    put(key, key_hbm, len(outs))

    for s in range(1, dp):
        src = lax.rem(d + s, dp)
        arrived(fin.at[src], rd_recv.at[src], dev(f, src))
    loads[4].wait()
    for h in range(2):
        total = fin[h]
        for g in range(1, dp // 2):
            total = total + fin[2 * g + h]
        cols = slice(h * half, (h + 1) * half)
        gb[:, cols] = main[:, cols] + total * scale
    put(gb, gb_hbm, len(outs))
    for cp in sent:
        cp.wait_send()
    for cp in outs:
        cp.wait()


def reorder_kernel(depth, scatter, order_ref, x_ref, y_ref):
    for j in range(x_ref.shape[1] // depth):
        here = slice(j * depth, (j + 1) * depth)
        there = pl.ds(pl.multiple_of(order_ref[j] * depth, depth), depth)
        if scatter:
            y_ref[:, there] = x_ref[:, here]
        else:
            y_ref[:, here] = x_ref[:, there]


def reorder(x, order, scatter):
    rows, width = x.shape
    n = order.shape[0]
    depth = width // n
    if depth % 128:
        if scatter:
            order = jnp.argsort(order)
        return jnp.take(x.reshape(rows, n, depth), order, axis=1, mode="clip").reshape(rows, width)
    tile = rows // 4
    spec = pl.BlockSpec((tile, width), lambda i: (i, 0))
    return pl.pallas_call(
        functools.partial(reorder_kernel, depth, scatter),
        grid=(rows // tile,),
        out_shape=jax.ShapeDtypeStruct((rows, width), x.dtype),
        in_specs=[pl.BlockSpec(memory_space=pltpu.SMEM), spec],
        out_specs=spec,
        cost_estimate=pl.CostEstimate(flops=0, bytes_accessed=4 * rows * width, transcendentals=0),
    )(order, x)


def exchange(
    n, dp, scale,
    order_hbm, x_hbm, c_hbm, w_hbm, main_hbm,
    key, ig, gb, order,
    xx, cc, ck, gath, mine, give, take, part, r1, hop, zin, t3, r3, fin, main, acc,
    load_sem, send_sem, ag_recv, b_recv, sib_recv, take_recv, r1_recv, z_recv, r3_recv, fin_recv,
):
    f = lax.axis_index("fsdp")
    d = lax.axis_index("dp")
    k = lax.rem(d, 2)
    sib = d + 1 - 2 * k
    chunk, key_width = main_hbm.shape
    half = key_width // 2
    part_rows = chunk // 2
    depth = n // 4
    z = lax.div(f, 4)
    low = lax.rem(f, 4)
    bit0 = lax.rem(low, 2)
    bit1 = lax.div(low, 2)
    flip0 = low + 1 - 2 * bit0
    flip1 = low + 2 - 4 * bit1
    low_a = flip0 + k * (flip1 - flip0)
    low_b = flip1 + k * (flip0 - flip1)
    low_ab = 3 - low
    lows = (low, low_a, low_b, low_ab)
    upper = lax.div(2 * z, depth)
    has_up = z < depth - 1
    has_dn = z > 0
    mid = jnp.logical_and(has_up, has_dn)

    def close(i):
        up = i + jnp.where(i >= z, 1, 0)
        dn = depth - 1 - i - jnp.where(depth - 1 - i <= z, 1, 0)
        return (1 - upper) * up + upper * dn

    def far(t):
        return close(depth - 2 - t) if t < depth - 1 else z

    def dev(fi, di):
        return {"fsdp": fi, "dp": di}

    to_a = dev(z * 4 + low_a, d)
    to_b = dev(z * 4 + low_b, d)
    to_sib = dev(f, sib)

    def level(zi):
        return dev(lax.rem(zi + depth, depth) * 4 + low, d)

    def load(src, dst, i):
        pltpu.make_async_copy(src, dst, load_sem.at[i]).start()

    load(w_hbm.at[:, pl.ds(0, half)], gath.at[0, z, 0], 0)
    load(w_hbm.at[:, pl.ds(half, half)], gath.at[1, z, 0], 0)
    load(order_hbm, order, 1)
    load(c_hbm, cc, 2)
    for j in range(n):
        load(x_hbm.at[:, pl.ds(j * chunk, chunk)], xx.at[j], 3)
    load(main_hbm, main, 4)

    barrier = pltpu.get_barrier_semaphore()

    def greet(to):
        pl.semaphore_signal(barrier, inc=1, device_id=to, device_id_type=MESH)

    greet(to_a)
    greet(to_b)
    for s in range(1, dp):
        greet(dev(f, lax.rem(d + s, dp)))

    @pl.when(has_up)
    def _():
        greet(level(z + 1))

    @pl.when(has_dn)
    def _():
        greet(level(z - 1))

    pl.semaphore_wait(barrier, dp + 1 + jnp.where(has_up, 1, 0) + jnp.where(has_dn, 1, 0))

    sent = []

    def send(src, dst, rsem, to, cond=None):
        cp = pltpu.make_async_remote_copy(
            src_ref=src, dst_ref=dst, send_sem=send_sem, recv_sem=rsem, device_id=to, device_id_type=MESH
        )
        if cond is None:
            cp.start()
        else:
            pl.when(cond)(cp.start)
        return cp, cond

    def post(*args):
        sent.append(send(*args))

    def arrived(dst, rsem):
        pltpu.make_async_remote_copy(
            src_ref=dst, dst_ref=dst, send_sem=send_sem, recv_sem=rsem, device_id=to_sib, device_id_type=MESH
        ).wait_recv()

    def rows_of(p):
        return pl.ds(p * part_rows, part_rows)

    def forward(zz, kind):
        send(gath.at[k, zz, kind], gath.at[k, zz, kind + 2], b_recv.at[kind, zz], to_b)

    def forward_piece(zz, kind, there, p, to, cond=None):
        src = gath.at[k, zz, kind, rows_of(p)]
        dst = gath.at[k, zz, there, rows_of(p)]
        send(src, dst, ag_recv.at[there, zz, p], to, cond)

    def forward_sib(zz, kind):
        send(gath.at[k, zz, kind], gath.at[k, zz, SWAP[kind]], sib_recv.at[SLOT[kind], zz], to_sib)

    contract_rows = (((0,), (0,)), ((), ()))
    contract_cols = (((1,), (1,)), ((), ()))

    def partial(kind, t):
        zz = far(t)
        prod = lax.dot_general(xx[order[zz * 4 + lows[kind]]], ck[...], contract_rows, preferred_element_type=F32)
        give[zz, kind] = prod[:, half:].astype(BF16)
        there = 3 - SWAP[kind]
        send(give.at[zz, kind], take.at[zz, there], take_recv.at[there // 2, zz], to_sib)
        mine[zz, kind] = prod[:, :half]

    def taken(group, zz):
        arrived(take.at[zz, pl.ds(2 * group, 2)], take_recv.at[group, zz])

    def pair(zz, kind, span):
        return mine[zz, kind, span] + take[zz, 3 - kind, span].astype(F32)

    def across(j, t):
        zz = far(t)
        if j:
            taken(0, zz)
        part[j, zz] = pair(zz, 2 + j, slice(None)).astype(BF16)
        send(part.at[j, zz], r1.at[j, zz], r1_recv.at[j, zz], to_b)

    def from_a(p):
        arrived(gath.at[k, z, 1, rows_of(p)], ag_recv.at[1, z, p])
        forward_piece(z, 1, 1, p, level(z + 1), has_up)
        forward_piece(z, 1, 1, p, level(z - 1), has_dn)
        if p:
            forward(z, 1)
            forward_sib(z, 1)

    def from_z(i, j, p):
        zz = close(i)
        arrived(gath.at[k, zz, j, rows_of(p)], ag_recv.at[j, zz, p])
        below = zz < z
        on = jnp.logical_or(jnp.logical_and(below, has_up), jnp.logical_and(zz > z, has_dn))
        forward_piece(zz, j, j, p, level(z + jnp.where(below, 1, -1)), on)
        if p:
            forward(zz, j)
            forward_sib(zz, j)

    def from_b(zz, j):
        arrived(gath.at[k, zz, 2 + j], b_recv.at[j, zz])
        forward_sib(zz, 2 + j)

    def ready(j, zz):
        if j:
            taken(1, zz)
        arrived(r1.at[j, zz], r1_recv.at[j, zz])

    def summed(j, zz, span):
        return pair(zz, j, span) + r1[j, zz, span].astype(F32)

    def along(t, j, p):
        zz = far(t)
        side = jnp.where(zz > z, 0, 1)
        edge = jnp.where(zz > z, z == 0, z == depth - 1)
        span = rows_of(p)
        spot = zin.at[side, zz, j, span]
        if not p:
            ready(j, zz)

        @pl.when(jnp.logical_not(edge))
        def _():
            arrived(spot, z_recv.at[zz, j, p])

        total = summed(j, zz, span) + spot[...].astype(F32)
        hop[j, zz, span] = total.astype(BF16)
        there = z + 1 - 2 * side
        slot = jnp.where(side * depth + zz == depth + there, depth, zz)
        send(hop.at[j, zz, span], spot, z_recv.at[slot, j, p], level(there))

    def settle(j, p):
        span = rows_of(p)
        if not p:
            ready(j, z)

        @pl.when(has_dn)
        def _():
            arrived(zin.at[0, z, j, span], z_recv.at[z, j, p])

        @pl.when(has_up)
        def _():
            arrived(zin.at[1, z, j, span], z_recv.at[depth, j, p])

        return summed(j, z, span) + zin[0, z, j, span].astype(F32) + zin[1, z, j, span].astype(F32)

    def use(zz, kind, first=False):
        fb = zz * 4 + lows[kind]
        w0 = gath[0, zz, kind]
        w1 = gath[1, zz, kind]
        prod = lax.dot_general(cc[:, :half], w0, contract_cols, preferred_element_type=F32)
        prod = prod + lax.dot_general(cc[:, half:], w1, contract_cols, preferred_element_type=F32)
        ig[fb] = prod.astype(BF16)
        xb = xx[order[fb]]
        k0 = jnp.dot(xb, w0, preferred_element_type=F32)
        k1 = jnp.dot(xb, w1, preferred_element_type=F32)
        if first:
            acc[:, :half] = k0
            acc[:, half:] = k1
        else:
            acc[:, :half] += k0
            acc[:, half:] += k1

    def use_when(zz, *kinds):
        arrived(gath.at[1 - k, zz, pl.ds(kinds[0], len(kinds))], sib_recv.at[SLOT[kinds[0]], zz])
        for kind in kinds:
            use(zz, kind)

    arrived(gath.at[:, z, 0], load_sem.at[0])
    for p in range(2):
        forward_piece(z, 0, 1, p, to_a)
        forward_piece(z, 0, 0, p, level(z + 1), has_up)
        forward_piece(z, 0, 0, p, level(z - 1), has_dn)

    forward(z, 0)

    @pl.when(z == 0)
    def _():
        zin[0] = jnp.zeros(zin.shape[1:], BF16)

    @pl.when(z == depth - 1)
    def _():
        zin[1] = jnp.zeros(zin.shape[1:], BF16)

    pltpu.make_async_copy(order_hbm, order, load_sem.at[1]).wait()
    pltpu.make_async_copy(c_hbm, cc, load_sem.at[2]).wait()
    arrived(xx, load_sem.at[3])
    ck[:, :half] = cc[:, pl.ds(pl.multiple_of(k * half, half), half)]
    ck[:, half:] = cc[:, pl.ds(pl.multiple_of((1 - k) * half, half), half)]
    def start(*tasks):
        for what, t in tasks:
            if what == "p":
                partial(3, t)
                partial(1, t)
                partial(2, t)
            else:
                across(1, t)
                across(0, t)

    start(("p", 0))
    start(("p", 1), ("s", 0))
    partial(0, 0)
    start(("p", 2))
    from_a(0)
    start(("s", 1))
    from_a(1)
    start(("p", 3), ("s", 2))
    for p in range(2):
        from_z(0, 0, p)

        @pl.when(mid)
        def _():
            from_z(1, 0, p)

    def both(fn, *args):
        fn(*args, 0)
        fn(*args, 1)

    partial(0, 1)

    @pl.when(jnp.logical_not(mid))
    def _():
        both(along, 0, 1)

    start(("s", 3))

    @pl.when(jnp.logical_not(mid))
    def _():
        partial(0, 2)
        both(along, 0, 0)
        both(from_z, 0, 1)
        both(along, 1, 1)
        partial(0, 3)
        use(z, 0, True)
        both(along, 1, 0)
        both(from_z, 1, 0)
        from_b(z, 0)
        use_when(close(0), 0)
        from_z(1, 1, 0)
        both(along, 2, 1)
        from_z(1, 1, 1)
        both(along, 2, 0)
        use_when(close(1), 0)
        both(from_z, 2, 0)
        from_b(z, 1)
        use_when(z, 1, 2)
        from_b(close(0), 0)
        both(from_z, 2, 1)

    @pl.when(mid)
    def _():
        partial(0, 2)
        from_z(0, 1, 0)
        from_z(1, 1, 0)
        from_z(0, 1, 1)
        from_z(1, 1, 1)
        partial(0, 3)
        use(z, 0, True)
        both(from_z, 2, 0)
        both(along, 0, 1)
        from_b(z, 0)
        use_when(close(0), 0)
        along(0, 0, 0)
        from_z(2, 1, 0)
        along(0, 0, 1)
        from_z(2, 1, 1)
        use_when(close(1), 0)
        both(along, 2, 1)
        both(along, 1, 1)
        from_b(z, 1)
        both(along, 2, 0)
        use_when(z, 1, 2)
        from_b(close(0), 0)
        both(along, 1, 0)

    use_when(close(2), 0)
    use_when(z, 3)
    for p in range(2):
        t3[rows_of(p)] = settle(1, p).astype(BF16)
        send(t3.at[rows_of(p)], r3.at[rows_of(p)], r3_recv.at[p], to_a)
    from_b(close(0), 1)
    use_when(close(0), 1, 2)
    from_b(close(1), 0)
    use_when(close(0), 3)
    from_b(close(1), 1)
    use_when(close(1), 1, 2)
    from_b(close(2), 0)
    use_when(close(1), 3)
    for p in range(2):
        fin[d, rows_of(p)] = settle(0, p)
    for p in range(2):
        arrived(r3.at[rows_of(p)], r3_recv.at[p])
        fin[d, rows_of(p)] += r3[rows_of(p)].astype(F32)
        own = fin.at[d, rows_of(p)]
        for s in range(1, dp):
            send(own, own, fin_recv.at[d, p], dev(f, lax.rem(d + s, dp)))
    from_b(close(2), 1)
    use_when(close(2), 1, 2)
    pltpu.make_async_copy(main_hbm, main, load_sem.at[4]).wait()
    for s in range(1, dp):
        src = lax.rem(d + s, dp)
        for p in range(2):
            arrived(fin.at[src, rows_of(p)], fin_recv.at[src, p])
    for h in range(2):
        total = fin[h]
        for g in range(1, dp // 2):
            total = total + fin[2 * g + h]
        side = slice(h * half, (h + 1) * half)
        gb[:, side] = main[:, side] + total * scale
    use_when(close(2), 3)
    key[...] = acc[...].astype(BF16)

    def send_done(src):
        pltpu.make_async_remote_copy(
            src_ref=src, dst_ref=src, send_sem=send_sem, recv_sem=r3_recv.at[0], device_id=to_sib, device_id_type=MESH
        ).wait_send()

    def left(_, carry):
        send_done(give.at[0, 0])
        return carry

    blocks = 4 + 6 * (depth - 1) + 8 * depth + 1
    for _ in range(blocks // n):
        send_done(give)
    per_z = jnp.where(has_up, z + 1, 0) + jnp.where(has_dn, depth - z, 0)
    lax.fori_loop(0, blocks % n + 2 * per_z, left, 0)
    for s in range(1, dp):
        send_done(fin.at[d])


def place(order, key, ig, gb, key_hbm, ig_hbm, gb_hbm, sem):
    n, _, chunk = ig.shape
    for fb in range(n):
        there = pl.ds(pl.multiple_of(order[fb] * chunk, chunk), chunk)
        pltpu.make_async_copy(ig.at[fb], ig_hbm.at[:, there], sem.at[0]).start()
    rest = [pltpu.make_async_copy(gb, gb_hbm, sem.at[1]), pltpu.make_async_copy(key, key_hbm, sem.at[2])]
    for cp in rest:
        cp.start()
    pltpu.make_async_copy(ig_hbm, ig_hbm, sem.at[0]).wait()
    for cp in rest:
        cp.wait()


def near(x, c, w, main, order, n, dp, scale):
    rows, width = x.shape
    chunk, key_width = main.shape
    half = key_width // 2
    depth = n // 4
    dma = pltpu.SemaphoreType.DMA
    block = (chunk, half)
    hbm = pl.BlockSpec(memory_space=pltpu.HBM)
    smem = pl.BlockSpec(memory_space=pltpu.SMEM)
    vmem = pl.BlockSpec(memory_space=pltpu.VMEM)
    operands = [pltpu.with_memory_space_constraint(a, pltpu.HBM) for a in (order, x, c, w, main)]
    key, ig, gb, order = pl.pallas_call(
        functools.partial(exchange, n, dp, scale),
        out_shape=(
            pltpu.VMEM((rows, key_width), BF16),
            pltpu.VMEM((n, rows, chunk), BF16),
            pltpu.VMEM((chunk, key_width), F32),
            pltpu.SMEM((n,), jnp.int32),
        ),
        in_specs=[hbm] * 5,
        out_specs=(vmem,) * 3 + (smem,),
        scratch_shapes=[
            pltpu.VMEM((n, rows, chunk), BF16),
            pltpu.VMEM((rows, key_width), BF16),
            pltpu.VMEM((rows, key_width), BF16),
            pltpu.VMEM((2, depth, 4) + block, BF16),
            pltpu.VMEM((depth, 4) + block, F32),
            pltpu.VMEM((depth, 4) + block, BF16),
            pltpu.VMEM((depth, 4) + block, BF16),
            pltpu.VMEM((2, depth) + block, BF16),
            pltpu.VMEM((2, depth) + block, BF16),
            pltpu.VMEM((2, depth) + block, BF16),
            pltpu.VMEM((2, depth, 2) + block, BF16),
            pltpu.VMEM(block, BF16),
            pltpu.VMEM(block, BF16),
            pltpu.VMEM((dp,) + block, F32),
            pltpu.VMEM((chunk, key_width), F32),
            pltpu.VMEM((rows, key_width), F32),
            dma((5,)),
            dma,
            dma((2, depth, 2)),
            dma((2, depth)),
            dma((3, depth)),
            dma((2, depth)),
            dma((2, depth)),
            dma((depth + 1, 2, 2)),
            dma((2,)),
            dma((dp, 2)),
        ],
        compiler_params=pltpu.CompilerParams(
            collective_id=0, has_side_effects=True, vmem_limit_bytes=36 * 1024 * 1024
        ),
    )(*operands)
    return pl.pallas_call(
        place,
        out_shape=(
            jax.ShapeDtypeStruct((rows, key_width), BF16),
            jax.ShapeDtypeStruct((rows, width), BF16),
            jax.ShapeDtypeStruct((chunk, key_width), F32),
        ),
        in_specs=[smem] + [vmem] * 3,
        out_specs=(hbm,) * 3,
        scratch_shapes=[dma((3,))],
        compiler_params=pltpu.CompilerParams(vmem_limit_bytes=8 * 1024 * 1024),
    )(order, key, ig, gb)


def body(normed, kv_cotangent, kv_weight, main_grad, owner_order):
    micro_count, tok_dev, width = normed.shape
    shard_rows, key_width = kv_weight.shape
    n = lax.axis_size("fsdp")
    dp = lax.axis_size("dp")
    rows = micro_count * tok_dev
    half = key_width // 2
    depth = n // 4
    scale = 1.0 / math.sqrt(rows * n * dp)
    chunk = shard_rows if shard_rows % 128 == 0 else max(shard_rows, 256)
    if depth == 4 and shard_rows % 128 == 0:
        key, ig, gb = near(
            normed.reshape(rows, width), kv_cotangent.reshape(rows, key_width), kv_weight, main_grad, owner_order, n, dp, scale
        )
        return (
            key.reshape(micro_count, tok_dev, key_width),
            ig.reshape(micro_count, tok_dev, width),
            gb,
        )
    x = reorder(normed.reshape(rows, width), owner_order, False)
    chunks = width // chunk
    dma = pltpu.SemaphoreType.DMA
    half_block = (shard_rows, half)
    any_spec = pl.BlockSpec(memory_space=pl.ANY)
    key, ig, gb = pl.pallas_call(
        functools.partial(kernel, n, dp, chunk, scale),
        out_shape=(
            jax.ShapeDtypeStruct((rows, key_width), BF16),
            jax.ShapeDtypeStruct((rows, width), BF16),
            jax.ShapeDtypeStruct((shard_rows, key_width), F32),
        ),
        in_specs=[any_spec] * 4,
        out_specs=(any_spec,) * 3,
        scratch_shapes=[
            pltpu.VMEM((2, rows, width), BF16),
            pltpu.VMEM((2, rows, key_width), BF16),
            pltpu.VMEM((2 * rows, half), BF16),
            pltpu.VMEM((2, n) + half_block, BF16),
            pltpu.VMEM((n,) + half_block, BF16),
            pltpu.VMEM((2, depth) + half_block, BF16),
            pltpu.VMEM((depth,) + half_block, BF16),
            pltpu.VMEM((depth,) + half_block, BF16),
            pltpu.VMEM((depth,) + half_block, BF16),
            pltpu.VMEM((depth,) + half_block, BF16),
            pltpu.VMEM((dp,) + half_block, F32),
            pltpu.VMEM((shard_rows, key_width), F32),
            pltpu.VMEM((shard_rows, key_width), F32),
            pltpu.VMEM((rows, key_width), BF16),
            pltpu.VMEM((rows, width), BF16),
            pltpu.VMEM((rows, key_width), F32),
            dma((5,)),
            dma((chunks + 2,)),
            dma,
            dma((2,)),
            dma((depth,)),
            dma((depth,)),
            dma((2 * depth,)),
            dma((n,)),
            dma((2, depth)),
            dma((depth,)),
            dma((depth,)),
            dma((dp,)),
        ],
        compiler_params=pltpu.CompilerParams(
            collective_id=0, has_side_effects=True
        ),
    )(x, kv_cotangent.reshape(rows, key_width), kv_weight, main_grad)
    ig = reorder(ig, owner_order, True)
    return (
        key.reshape(micro_count, tok_dev, key_width),
        ig.reshape(micro_count, tok_dev, width),
        gb,
    )


def solution(mesh):
    in_specs = (
        P(None, ("fsdp", "dp"), None),
        P(None, ("fsdp", "dp"), None),
        P("fsdp", None),
        P("fsdp", None),
        P(),
    )
    out_specs = (P(None, ("fsdp", "dp"), None), P(None, ("fsdp", "dp"), None), P("fsdp", None))
    return jax.shard_map(body, mesh=mesh, in_specs=in_specs, out_specs=out_specs, check_vma=False)
```
